128 devices in a mesh: dp: 1, tp: 2 (over core), cp: 64 (over z, y, x).
Axes of the slice: x: 4, y: 4, z: 4, core: 2. Of those that a mesh axis runs over, the one named last changes fastest.
Arguments:
- tokens: bfloat16 [12288, 3072], P(('dp', 'tp', 'cp'))
- norm_attn: bfloat16 [2, 3072], replicated
- norm_mlp: bfloat16 [2, 3072], replicated
- w_q: bfloat16 [2, 3072, 24, 128], P(None, None, 'tp')
- w_k: bfloat16 [2, 3072, 1024], P(None, None, 'tp')
- w_v: bfloat16 [2, 3072, 1024], P(None, None, 'tp')
- w_o: bfloat16 [2, 24, 128, 3072], P(None, 'tp')
- w_gate: bfloat16 [2, 3072, 8192], P(None, None, 'tp')
- w_up: bfloat16 [2, 3072, 8192], P(None, None, 'tp')
- w_down: bfloat16 [2, 8192, 3072], P(None, 'tp')
Outputs:
- output: bfloat16 [12288, 3072], P(('dp', 'tp', 'cp'))
All inputs are finite; a program needn't handle non-finite values.
Results may differ from the reference program's by a relative error of at most 0.02.
Values are sent between devices in bfloat16 or wider.
A program may use at most 1 GiB of HBM per device.

```python
import math
import jax
import jax.numpy as jnp
from jax import lax

D = 3072
FF = 8192
HEADS = 24
KV_HEADS = 8
HEAD = 128
SEQ = 12288
SEGMENT = 48
LAYERS = 2

GROUP = HEADS // KV_HEADS
GROUP_DEVICES = SEQ // (2 * SEGMENT)


def row_positions():
    row_idx = jnp.arange(SEQ)
    device_idx = row_idx // (2 * SEGMENT)
    offset = row_idx % (2 * SEGMENT)
    seg_idx = jnp.where(offset < SEGMENT, device_idx, 2 * GROUP_DEVICES - 1 - device_idx)
    return seg_idx * SEGMENT + offset % SEGMENT


def rms_norm(hidden, gain):
    hidden_f = hidden.astype(jnp.float32)
    inv_rms = lax.rsqrt(jnp.mean(hidden_f * hidden_f, axis=-1, keepdims=True) + 1e-5)
    return (hidden_f * inv_rms * gain.astype(jnp.float32)).astype(jnp.bfloat16)


def rotary(values, positions):
    half_dim = values.shape[-1] // 2
    inv_freq = 500000.0 ** (-(jnp.arange(half_dim, dtype=jnp.float32) * 2.0 / values.shape[-1]))
    angles = positions.astype(jnp.float32)[:, None] * inv_freq[None, :]
    cos_ang = jnp.cos(angles)[:, None, :]
    sin_ang = jnp.sin(angles)[:, None, :]
    first = values[..., :half_dim]
    second = values[..., half_dim:]
    return jnp.concatenate([first * cos_ang - second * sin_ang, second * cos_ang + first * sin_ang], axis=-1)


def attention(queries, keys, value_rows, positions):
    keys_f = keys.astype(jnp.float32)
    values_f = value_rows.astype(jnp.float32)
    q_blocks = queries.reshape(SEQ // SEGMENT, SEGMENT, KV_HEADS, GROUP, HEAD)
    pos_blocks = positions.reshape(SEQ // SEGMENT, SEGMENT)
    scale = 1.0 / math.sqrt(HEAD)

    def one_block(block):
        q_blk, pos_blk = block
        scores = jnp.einsum('bkgd,tkd->bkgt', q_blk.astype(jnp.float32), keys_f) * scale
        visible = positions[None, None, None, :] <= pos_blk[:, None, None, None]
        scores = jnp.where(visible, scores, -jnp.inf)
        row_max = jnp.max(scores, axis=-1, keepdims=True)
        weights = jnp.exp(scores - row_max)
        row_sum = jnp.sum(weights, axis=-1, keepdims=True)
        mixed = jnp.einsum('bkgt,tkd->bkgd', weights.astype(jnp.bfloat16).astype(jnp.float32), values_f)
        return (mixed / row_sum).astype(jnp.bfloat16)

    return lax.map(one_block, (q_blocks, pos_blocks)).reshape(SEQ, HEADS * HEAD)


def layer(hidden, params, positions):
    norm_attn, norm_mlp, w_q, w_k, w_v, w_o, w_gate, w_up, w_down = params
    normed = rms_norm(hidden, norm_attn)
    q_proj = jnp.dot(normed, w_q.reshape(D, HEADS * HEAD), preferred_element_type=jnp.float32)
    queries = rotary(q_proj.reshape(SEQ, HEADS, HEAD), positions).astype(jnp.bfloat16)
    k_proj = jnp.dot(normed, w_k, preferred_element_type=jnp.float32)
    keys = rotary(k_proj.reshape(SEQ, KV_HEADS, HEAD), positions).astype(jnp.bfloat16)
    value_rows = jnp.dot(normed, w_v, preferred_element_type=jnp.float32).astype(jnp.bfloat16).reshape(SEQ, KV_HEADS, HEAD)
    mixed = attention(queries.reshape(SEQ, KV_HEADS, GROUP, HEAD), keys, value_rows, positions)
    attn_out = jnp.dot(mixed, w_o.reshape(HEADS * HEAD, D), preferred_element_type=jnp.float32)
    hidden_mid = (hidden.astype(jnp.float32) + attn_out).astype(jnp.bfloat16)
    normed_mlp = rms_norm(hidden_mid, norm_mlp)
    gate_pre = jnp.dot(normed_mlp, w_gate, preferred_element_type=jnp.float32)
    up_proj = jnp.dot(normed_mlp, w_up, preferred_element_type=jnp.float32)
    hidden_act = (jax.nn.silu(gate_pre) * up_proj).astype(jnp.bfloat16)
    mlp_out = jnp.dot(hidden_act, w_down, preferred_element_type=jnp.float32)
    return (hidden_mid.astype(jnp.float32) + mlp_out).astype(jnp.bfloat16)


def setup_inputs(seed: int = 0, part: int = 0) -> dict:
    key_list = jax.random.split(jax.random.key(seed), 10)
    score_gain = math.sqrt(max(math.log(SEQ) - 2.0, 1.0))
    tokens = jax.random.normal(jax.random.fold_in(key_list[0], part), (SEQ, D), jnp.float32)
    norm_attn = 1.0 + 0.3 * jax.random.normal(key_list[1], (LAYERS, D), jnp.float32)
    norm_mlp = 1.0 + 0.3 * jax.random.normal(key_list[2], (LAYERS, D), jnp.float32)
    w_q = jax.random.normal(key_list[3], (LAYERS, D, HEADS, HEAD), jnp.float32) * (score_gain / math.sqrt(D))
    w_k = jax.random.normal(key_list[4], (LAYERS, D, KV_HEADS * HEAD), jnp.float32) / math.sqrt(D)
    w_v = jax.random.normal(key_list[5], (LAYERS, D, KV_HEADS * HEAD), jnp.float32) / math.sqrt(D)
    w_o = jax.random.normal(key_list[6], (LAYERS, HEADS, HEAD, D), jnp.float32) / math.sqrt(HEADS * HEAD)
    w_gate = jax.random.normal(key_list[7], (LAYERS, D, FF), jnp.float32) / math.sqrt(D)
    w_up = jax.random.normal(key_list[8], (LAYERS, D, FF), jnp.float32) / math.sqrt(D)
    w_down = jax.random.normal(key_list[9], (LAYERS, FF, D), jnp.float32) * (1.5 / math.sqrt(FF))
    return dict(
        tokens=tokens.astype(jnp.bfloat16),
        norm_attn=norm_attn.astype(jnp.bfloat16),
        norm_mlp=norm_mlp.astype(jnp.bfloat16),
        w_q=w_q.astype(jnp.bfloat16),
        w_k=w_k.astype(jnp.bfloat16),
        w_v=w_v.astype(jnp.bfloat16),
        w_o=w_o.astype(jnp.bfloat16),
        w_gate=w_gate.astype(jnp.bfloat16),
        w_up=w_up.astype(jnp.bfloat16),
        w_down=w_down.astype(jnp.bfloat16),
    )


def reference(tokens, norm_attn, norm_mlp, w_q, w_k, w_v, w_o, w_gate, w_up, w_down):
    positions = row_positions()

    def layer_step(hidden, params):
        return layer(hidden, params, positions), None

    stacked = (norm_attn, norm_mlp, w_q, w_k, w_v, w_o, w_gate, w_up, w_down)
    return lax.scan(layer_step, tokens, stacked)[0]
```

```python
import functools
import math
import jax
import jax.numpy as jnp
from jax import lax
from jax.experimental import pallas as pl
from jax.experimental.pallas import tpu as pltpu
from jax.sharding import Mesh, PartitionSpec as P

SEG = 48
HD = 128
GRP = 3
XN = 4
SN = 16
RUN = XN * SEG
NRUN = 4
CH = NRUN * RUN


def rms_norm(hidden, gain):
    hidden_f = hidden.astype(jnp.float32)
    inv_rms = lax.rsqrt(jnp.mean(hidden_f * hidden_f, axis=-1, keepdims=True) + 1e-5)
    return (hidden_f * inv_rms * gain.astype(jnp.float32)).astype(jnp.bfloat16)


def seg_positions(dev_ids, rows, dev_total):
    offset = jnp.arange(rows)
    half_len = rows // 2
    seg_idx = jnp.where(offset < half_len, dev_ids[..., None], 2 * dev_total - 1 - dev_ids[..., None])
    return seg_idx * half_len + offset % half_len


def flash_kernel(q_ref, kv_ref, o_ref):
    group = lax.axis_index('z') * 4 + lax.axis_index('y')
    scale = math.log2(math.e) / math.sqrt(HD)

    def quarter_block(quarter):
        return jnp.where(quarter == 0, 0, jnp.where(quarter == 1, 2, jnp.where(quarter == 2, 3, 1)))

    def one_quarter(quarter, carry):
        blk = quarter_block(quarter)
        desc = quarter >= 2
        order = quarter * SN + jnp.where(desc, SN - 1 - group, group)
        xs = [jnp.where(desc, XN - 1 - i, i) for i in range(XN)]
        qs = [jnp.concatenate([q_ref[x, blk, :, h * HD:(h + 1) * HD] for x in xs], axis=0) for h in range(GRP)]

        def chunk(c, state, masked):
            kq = c // (SN // NRUN)
            kblk = quarter_block(kq)
            kdesc = kq >= 2
            parts_k, parts_v = [], []
            for r in range(NRUN):
                idx = (c % (SN // NRUN)) * NRUN + r
                member = jnp.where(kdesc, SN - 1 - idx, idx)
                for i in range(XN):
                    x = jnp.where(kdesc, XN - 1 - i, i)
                    parts_k.append(kv_ref[member, x, kblk, :, :HD])
                    parts_v.append(kv_ref[member, x, kblk, :, HD:])
            keys = jnp.concatenate(parts_k, axis=0)
            vals = jnp.concatenate(parts_v, axis=0)
            out = []
            if masked:
                row = lax.broadcasted_iota(jnp.int32, (RUN, CH), 0)
                col = lax.broadcasted_iota(jnp.int32, (RUN, CH), 1)
                visible = col <= row + (order - c * NRUN) * RUN
            for h in range(GRP):
                m, l, acc = state[h]
                s = lax.dot_general(qs[h], keys, (((1,), (1,)), ((), ())), preferred_element_type=jnp.float32)
                if masked:
                    s = jnp.where(visible, s, -jnp.inf)
                m_new = jnp.maximum(m, jnp.max(s, axis=-1, keepdims=True))
                e = jnp.exp2((s - m_new) * scale)
                alpha = jnp.exp2((m - m_new) * scale)
                l_new = l * alpha + jnp.sum(e, axis=-1, keepdims=True)
                pv = jnp.dot(e.astype(jnp.bfloat16), vals, preferred_element_type=jnp.float32)
                out.append((m_new, l_new, acc * alpha + pv))
            return tuple(out)

        last = order // NRUN
        init = tuple((jnp.full((RUN, 1), -jnp.inf, jnp.float32), jnp.zeros((RUN, 1), jnp.float32),
                      jnp.zeros((RUN, HD), jnp.float32)) for _ in range(GRP))
        state = chunk(last, init, True)
        state = lax.fori_loop(0, last, lambda c, st: chunk(c, st, False), state)
        for h in range(GRP):
            m, l, acc = state[h]
            o = (acc / l).astype(jnp.bfloat16)
            for i in range(XN):
                o_ref[xs[i], blk, :, h * HD:(h + 1) * HD] = o[i * SEG:(i + 1) * SEG]
        return carry

    lax.fori_loop(0, 4, one_quarter, 0)


def flash(q, kv):
    return pl.pallas_call(
        flash_kernel,
        out_shape=jax.ShapeDtypeStruct(q.shape, jnp.bfloat16),
        in_specs=[pl.BlockSpec(memory_space=pltpu.VMEM)] * 2,
        out_specs=pl.BlockSpec(memory_space=pltpu.VMEM),
        compiler_params=pltpu.CompilerParams(vmem_limit_bytes=40 << 20),
        cost_estimate=pl.CostEstimate(flops=2 * 2 * 130 * 192 * 576 * 128, bytes_accessed=8 << 20, transcendentals=0),
        name='flash',
    )(q, kv)


def solution(mesh):
    tp_size = mesh.shape['tp']
    cp_size = mesh.shape['cp']
    dev_total = tp_size * cp_size
    mesh5 = Mesh(mesh.devices.reshape(1, tp_size, 4, 4, 4), ('dp', 'tp', 'z', 'y', 'x'))
    row_spec = P(('dp', 'tp', 'z', 'y', 'x'), None)
    gain_spec = P(None, None)
    q_spec = P(None, None, 'tp', None)
    col_spec = P(None, None, 'tp')
    o_spec = P(None, 'tp', None, None)
    down_spec = P(None, 'tp', None)

    def body(tokens, norm_attn, norm_mlp, w_q, w_k, w_v, w_o, w_gate, w_up, w_down):
        rows = tokens.shape[0]
        toks = tp_size * rows
        cp_idx = (lax.axis_index('z') * 4 + lax.axis_index('y')) * 4 + lax.axis_index('x')
        tp_devs = jnp.arange(tp_size) * cp_size + cp_idx
        pos = seg_positions(tp_devs, rows, dev_total).reshape(toks)
        inv_freq = 500000.0 ** (-(jnp.arange(HD // 2, dtype=jnp.float32) * 2.0 / HD))
        angles = pos.astype(jnp.float32)[:, None] * inv_freq[None, :]
        cos_a = jnp.cos(angles)[:, None, :]
        sin_a = jnp.sin(angles)[:, None, :]

        def rotary(v):
            a, b = v[..., :HD // 2], v[..., HD // 2:]
            return jnp.concatenate([a * cos_a - b * sin_a, b * cos_a + a * sin_a], axis=-1)

        hidden = tokens
        for layer in range(w_q.shape[0]):
            normed = lax.all_gather(rms_norm(hidden, norm_attn[layer]), 'tp', axis=0, tiled=True)
            q_proj = jnp.einsum('rd,dhe->rhe', normed, w_q[layer], preferred_element_type=jnp.float32)
            q = rotary(q_proj).astype(jnp.bfloat16).reshape(toks, XN, GRP * HD)
            k_proj = jnp.dot(normed, w_k[layer], preferred_element_type=jnp.float32)
            k = rotary(k_proj.reshape(toks, XN, HD)).astype(jnp.bfloat16)
            v = jnp.dot(normed, w_v[layer], preferred_element_type=jnp.float32).astype(jnp.bfloat16).reshape(toks, XN, HD)
            send = jnp.concatenate([q, k, v], axis=-1).transpose(1, 0, 2)
            got = lax.all_to_all(send, 'x', split_axis=0, concat_axis=0, tiled=True)
            q_own = got[:, :, :GRP * HD].reshape(XN, 4, SEG, GRP * HD)
            kv_own = got[:, :, GRP * HD:].reshape(XN, 4, SEG, 2 * HD)
            kv_all = lax.all_gather(kv_own, ('z', 'y'), axis=0, tiled=False)
            o_own = flash(q_own, kv_all.reshape(SN, XN, 4, SEG, 2 * HD))
            o = lax.all_to_all(o_own.reshape(XN, toks, GRP * HD), 'x', split_axis=0, concat_axis=0, tiled=True)
            attn_part = jnp.einsum('xre,xed->rd', o, w_o[layer].reshape(XN, GRP * HD, -1), preferred_element_type=jnp.float32)
            attn_out = lax.psum_scatter(attn_part, 'tp', scatter_dimension=0, tiled=True)
            hidden_mid = (hidden.astype(jnp.float32) + attn_out).astype(jnp.bfloat16)
            normed_mlp = lax.all_gather(rms_norm(hidden_mid, norm_mlp[layer]), 'tp', axis=0, tiled=True)
            gate = jnp.dot(normed_mlp, w_gate[layer], preferred_element_type=jnp.float32)
            up = jnp.dot(normed_mlp, w_up[layer], preferred_element_type=jnp.float32)
            act = (jax.nn.silu(gate) * up).astype(jnp.bfloat16)
            mlp_part = jnp.dot(act, w_down[layer], preferred_element_type=jnp.float32)
            mlp_out = lax.psum_scatter(mlp_part, 'tp', scatter_dimension=0, tiled=True)
            hidden = (hidden_mid.astype(jnp.float32) + mlp_out).astype(jnp.bfloat16)
        return hidden

    return jax.shard_map(
        body,
        mesh=mesh5,
        in_specs=(row_spec, gain_spec, gain_spec, q_spec, col_spec, col_spec, o_spec, col_spec, col_spec, down_spec),
        out_specs=row_spec,
        check_vma=False,
    )
```

```python
import functools
import math
import jax
import jax.numpy as jnp
from jax import lax
from jax.experimental import pallas as pl
from jax.experimental.pallas import tpu as pltpu
from jax.sharding import Mesh, PartitionSpec as P

def rms_norm(hidden, gain):
    hidden_f = hidden.astype(jnp.float32)
    inv_rms = lax.rsqrt(jnp.mean(hidden_f * hidden_f, axis=-1, keepdims=True) + 1e-5)
    return (hidden_f * inv_rms * gain.astype(jnp.float32)).astype(jnp.bfloat16)


def seg_positions(dev_ids, rows, dev_total):
    offset = jnp.arange(rows)
    half_len = rows // 2
    seg_idx = jnp.where(offset < half_len, dev_ids[..., None], 2 * dev_total - 1 - dev_ids[..., None])
    return seg_idx * half_len + offset % half_len


SEG = 48
HD = 128
GRP = 3
XN = 4
SN = 16
RUN = XN * SEG
NRUN = 4
CH = NRUN * RUN
QR = GRP * RUN
TOK = 192
SCALE = math.log2(math.e) / math.sqrt(HD)
NB = 20


def quarter_block(quarter):
    return jnp.where(quarter == 0, 0, jnp.where(quarter == 1, 2, jnp.where(quarter == 2, 3, 1)))


def attn_kernel(q_send, kv_send, o_out, q_own, kv_all, o_own, o_recv, s_a, s_b, mx_a, mx_b, m_ref, l_ref, acc_ref,
                send_a, recv_a, send_b, recv_b, send_o, recv_o, local_sem):
    zi, yi, xi = lax.axis_index('z'), lax.axis_index('y'), lax.axis_index('x')
    group = zi * 4 + yi

    def slot(coords):
        return coords[0] * 4 + coords[1]

    def plus(v, d):
        return lax.rem(v + d + 4, 4)

    barrier = pltpu.get_barrier_semaphore()
    for d in (1, 2, 3):
        pl.semaphore_signal(barrier, inc=1, device_id={'x': plus(xi, d)}, device_id_type=pl.DeviceIdType.MESH)
    for d in (1, -1):
        pl.semaphore_signal(barrier, inc=1, device_id={'y': plus(yi, d)}, device_id_type=pl.DeviceIdType.MESH)
        pl.semaphore_signal(barrier, inc=1, device_id={'z': plus(zi, d)}, device_id_type=pl.DeviceIdType.MESH)
    own_q = pltpu.make_async_copy(q_send.at[xi], q_own.at[xi], local_sem.at[0])
    own_kv = pltpu.make_async_copy(kv_send.at[xi], kv_all.at[group, xi], local_sem.at[1])
    own_q.start()
    own_kv.start()
    pl.semaphore_wait(barrier, 7)

    def remote(src, dst, ssem, rsem, dev):
        return pltpu.make_async_remote_copy(src_ref=src, dst_ref=dst, send_sem=ssem, recv_sem=rsem, device_id=dev,
                                            device_id_type=pl.DeviceIdType.MESH)

    kv_msgs, q_msgs = [], []
    for d in (1, 2, 3):
        to = plus(xi, d)
        kv_msgs.append(remote(kv_send.at[to], kv_all.at[group, xi], send_a.at[d - 1], recv_a.at[d - 1], {'x': to}))
        q_msgs.append(remote(q_send.at[to], q_own.at[xi], send_a.at[d + 2], recv_a.at[d + 2], {'x': to}))
    for c in kv_msgs:
        c.start()
    for c in q_msgs:
        c.start()
    own_kv.wait()
    for c in kv_msgs:
        c.wait_recv()

    pos = (zi, yi)
    names = ('z', 'y')

    def at(axis, da, db):
        other = 1 - axis
        c = [None, None]
        c[axis] = plus(pos[axis], da)
        c[other] = plus(pos[other], db)
        return slot(c)

    def msg(half, idx, where, part, axis, d):
        base = half * 2
        lo, n = (base, 2) if part is None else (base + part, 1)
        ref = kv_all.at[where, pl.ds(lo, n)]
        k = half * NB + idx
        return remote(ref, ref, send_b.at[k], recv_b.at[k], {names[axis]: plus(pos[axis], d)})

    first = (1, 0)
    stage = [dict() for _ in range(2)]
    offs = (0, -1, 1, 2)

    def begin(half, key, m):
        stage[half][key] = m
        m.start()

    def send_second(half, j):
        a = first[half]
        b = 1 - a
        for s, d in enumerate((1, -1)):
            begin(half, ('b', j, d), msg(half, 4 + j * 4 + s, at(a, offs[j], 0), None, b, d))

    def forward_second(half, j):
        a = first[half]
        b = 1 - a
        for s, d in enumerate((1, -1)):
            stage[half][('b', j, d)].wait_recv()
            begin(half, ('f', j, d), msg(half, 4 + j * 4 + 2 + s, at(a, offs[j], -d), s, b, d))

    for half in range(2):
        a = first[half]
        for s, d in enumerate((1, -1)):
            begin(half, ('a', d), msg(half, s, group, None, a, d))
    for half in range(2):
        send_second(half, 0)
    for half in range(2):
        a = first[half]
        for s, d in enumerate((1, -1)):
            stage[half][('a', d)].wait_recv()
            begin(half, ('g', d), msg(half, 2 + s, at(a, -d, 0), s, a, d))
    for half in range(2):
        send_second(half, 1)
        send_second(half, 2)
    for half in range(2):
        forward_second(half, 0)
    for half in range(2):
        for d in (1, -1):
            stage[half][('g', d)].wait_recv()
        send_second(half, 3)
    for j in (1, 2, 3):
        for half in range(2):
            forward_second(half, j)
    own_q.wait()
    for c in q_msgs:
        c.wait_recv()
    for half in range(2):
        for j in range(4):
            for d in (1, -1):
                stage[half][('f', j, d)].wait_recv()

    def flash_quarter(step, carry):
        quarter = 3 - step
        blk = quarter_block(quarter)
        row0 = pl.multiple_of(blk * SEG, 16)
        desc = quarter >= 2
        order = quarter * SN + jnp.where(desc, SN - 1 - group, group)
        last = order // NRUN
        xs = [jnp.where(desc, XN - 1 - i, i) for i in range(XN)]
        qs = jnp.concatenate([q_own[x, h, pl.ds(row0, SEG), :] for h in range(GRP) for x in xs], axis=0)

        def load(c, which):
            kq = c // (SN // NRUN)
            krow = pl.multiple_of(quarter_block(kq) * SEG, 16)
            kdesc = kq >= 2
            parts = []
            for r in range(NRUN):
                idx = (c % (SN // NRUN)) * NRUN + r
                member = jnp.where(kdesc, SN - 1 - idx, idx)
                for i in range(XN):
                    x = jnp.where(kdesc, XN - 1 - i, i)
                    parts.append(kv_all[member, x, which, pl.ds(krow, SEG), :])
            return jnp.concatenate(parts, axis=0)

        def qk(c, s_ref, mx_ref, masked):
            s = lax.dot_general(qs, load(c, 0), (((1,), (1,)), ((), ())), preferred_element_type=jnp.float32)
            if masked:
                row = lax.broadcasted_iota(jnp.int32, (RUN, CH), 0)
                col = lax.broadcasted_iota(jnp.int32, (RUN, CH), 1)
                visible = col <= row + (order - c * NRUN) * RUN
                s = jnp.concatenate([jnp.where(visible, s[h * RUN:(h + 1) * RUN], -jnp.inf) for h in range(GRP)], axis=0)
            s_ref[...] = s
            mx_ref[...] = jnp.broadcast_to(jnp.max(s, axis=-1, keepdims=True), (QR, HD))

        def soft(c, s_ref, mx_ref, valid):
            vals = load(c, 1)
            for h in range(GRP):
                rows = pl.ds(h * RUN, RUN)
                m_old = m_ref[rows, :]
                mx = mx_ref[rows, :]
                if valid is not None:
                    mx = jnp.where(valid, mx, -jnp.inf)
                m_new = jnp.maximum(m_old, mx)
                alpha = jnp.exp2((m_old - m_new) * SCALE)
                bias = m_new * SCALE
                if valid is not None:
                    bias = jnp.where(valid, bias, jnp.inf)
                lsum = l_ref[rows, :] * alpha
                es = []
                for t in range(CH // HD):
                    e = jnp.exp2(s_ref[rows, t * HD:(t + 1) * HD] * SCALE - bias)
                    lsum = lsum + e
                    es.append(e.astype(jnp.bfloat16))
                pv = jnp.dot(jnp.concatenate(es, axis=1), vals, preferred_element_type=jnp.float32)
                acc_ref[rows, :] = acc_ref[rows, :] * alpha + pv
                l_ref[rows, :] = lsum
                m_ref[rows, :] = m_new

        m_ref[...] = jnp.full((QR, HD), -jnp.inf, jnp.float32)
        l_ref[...] = jnp.zeros((QR, HD), jnp.float32)
        acc_ref[...] = jnp.zeros((QR, HD), jnp.float32)
        qk(last, s_a, mx_a, True)

        def pair(p, carry):
            c_cur = jnp.where(p == 0, last, 2 * p - 1)
            c_b = jnp.minimum(2 * p, last)
            c_a = jnp.minimum(2 * p + 1, last)
            qk(c_b, s_b, mx_b, False)
            soft(c_cur, s_a, mx_a, None)
            qk(c_a, s_a, mx_a, False)
            soft(c_b, s_b, mx_b, 2 * p < last)
            return carry

        lax.fori_loop(0, (last + 2) // 2, pair, 0)
        for h in range(GRP):
            rows = pl.ds(h * RUN, RUN)
            o = (acc_ref[rows, :] / jnp.sum(l_ref[rows, :], axis=-1, keepdims=True)).astype(jnp.bfloat16)
            for i in range(XN):
                o_own[xs[i], blk, h, :, :] = o[i * SEG:(i + 1) * SEG]
        for d in (1, 2, 3):
            to = plus(xi, d)
            remote(o_own.at[to, blk], o_recv.at[xi, blk], send_o.at[step, d - 1], recv_o.at[step, d - 1], {'x': to}).start()
        return carry

    lax.fori_loop(0, 4, flash_quarter, 0)
    o_recv[xi] = o_own[xi]
    for step in range(4):
        blk = (1, 3, 2, 0)[step]
        for d in (1, 2, 3):
            to = plus(xi, d)
            c = remote(o_own.at[to, blk], o_recv.at[xi, blk], send_o.at[step, d - 1], recv_o.at[step, d - 1], {'x': to})
            c.wait_send()
            c.wait_recv()
    o_out[...] = o_recv[...]
    for c in kv_msgs + q_msgs:
        c.wait_send()
    for half in range(2):
        for c in stage[half].values():
            c.wait_send()


def attention(q_send, kv_send):
    f32 = jnp.float32
    bf16 = jnp.bfloat16
    return pl.pallas_call(
        attn_kernel,
        out_shape=jax.ShapeDtypeStruct((XN, 4, GRP, SEG, HD), bf16),
        in_specs=[pl.BlockSpec(memory_space=pltpu.HBM)] * 2,
        out_specs=pl.BlockSpec(memory_space=pltpu.VMEM),
        scratch_shapes=[
            pltpu.VMEM((XN, GRP, TOK, HD), bf16),
            pltpu.VMEM((SN, XN, 2, TOK, HD), bf16),
            pltpu.VMEM((XN, 4, GRP, SEG, HD), bf16),
            pltpu.VMEM((XN, 4, GRP, SEG, HD), bf16),
            pltpu.VMEM((QR, CH), f32),
            pltpu.VMEM((QR, CH), f32),
            pltpu.VMEM((QR, HD), f32),
            pltpu.VMEM((QR, HD), f32),
            pltpu.VMEM((QR, HD), f32),
            pltpu.VMEM((QR, HD), f32),
            pltpu.VMEM((QR, HD), f32),
            pltpu.SemaphoreType.DMA((6,)),
            pltpu.SemaphoreType.DMA((6,)),
            pltpu.SemaphoreType.DMA((2 * NB,)),
            pltpu.SemaphoreType.DMA((2 * NB,)),
            pltpu.SemaphoreType.DMA((4, 3)),
            pltpu.SemaphoreType.DMA((4, 3)),
            pltpu.SemaphoreType.DMA((2,)),
        ],
        compiler_params=pltpu.CompilerParams(vmem_limit_bytes=40 << 20, collective_id=1, has_side_effects=True),
        cost_estimate=pl.CostEstimate(flops=2 * 2 * 130 * 192 * 576 * 128, bytes_accessed=8 << 20, transcendentals=0),
        name='attn',
    )(q_send, kv_send)


def solution(mesh):
    tp_size = mesh.shape['tp']
    cp_size = mesh.shape['cp']
    dev_total = tp_size * cp_size
    mesh5 = Mesh(mesh.devices.reshape(1, tp_size, 4, 4, 4), ('dp', 'tp', 'z', 'y', 'x'))
    row_spec = P(('dp', 'tp', 'z', 'y', 'x'), None)
    gain_spec = P(None, None)
    q_spec = P(None, None, 'tp', None)
    col_spec = P(None, None, 'tp')
    o_spec = P(None, 'tp', None, None)
    down_spec = P(None, 'tp', None)

    def body(tokens, norm_attn, norm_mlp, w_q, w_k, w_v, w_o, w_gate, w_up, w_down):
        rows = tokens.shape[0]
        toks = tp_size * rows
        cp_idx = (lax.axis_index('z') * 4 + lax.axis_index('y')) * 4 + lax.axis_index('x')
        tp_devs = jnp.arange(tp_size) * cp_size + cp_idx
        pos = seg_positions(tp_devs, rows, dev_total).reshape(toks)
        inv_freq = 500000.0 ** (-(jnp.arange(HD // 2, dtype=jnp.float32) * 2.0 / HD))
        angles = pos.astype(jnp.float32)[:, None] * inv_freq[None, :]
        cos_a = jnp.cos(angles)[None]
        sin_a = jnp.sin(angles)[None]

        def rotary(v):
            a, b = v[..., :HD // 2], v[..., HD // 2:]
            return jnp.concatenate([a * cos_a - b * sin_a, b * cos_a + a * sin_a], axis=-1)

        hidden = tokens
        for layer in range(w_q.shape[0]):
            normed = lax.all_gather(rms_norm(hidden, norm_attn[layer]), 'tp', axis=0, tiled=True)
            q_proj = jnp.einsum('rd,dhe->hre', normed, w_q[layer], preferred_element_type=jnp.float32)
            q_send = rotary(q_proj).astype(jnp.bfloat16).reshape(XN, GRP, toks, HD)
            k_proj = jnp.einsum('rd,dhe->hre', normed, w_k[layer].reshape(-1, XN, HD), preferred_element_type=jnp.float32)
            v_proj = jnp.einsum('rd,dhe->hre', normed, w_v[layer].reshape(-1, XN, HD), preferred_element_type=jnp.float32)
            kv_send = jnp.stack([rotary(k_proj).astype(jnp.bfloat16), v_proj.astype(jnp.bfloat16)], axis=1)
            o = attention(q_send, kv_send)
            o = o.transpose(1, 3, 0, 2, 4).reshape(toks, XN * GRP * HD)
            attn_part = jnp.dot(o, w_o[layer].reshape(XN * GRP * HD, -1), preferred_element_type=jnp.float32)
            attn_out = lax.psum_scatter(attn_part, 'tp', scatter_dimension=0, tiled=True)
            hidden_mid = (hidden.astype(jnp.float32) + attn_out).astype(jnp.bfloat16)
            normed_mlp = lax.all_gather(rms_norm(hidden_mid, norm_mlp[layer]), 'tp', axis=0, tiled=True)
            gate = jnp.dot(normed_mlp, w_gate[layer], preferred_element_type=jnp.float32)
            up = jnp.dot(normed_mlp, w_up[layer], preferred_element_type=jnp.float32)
            act = (jax.nn.silu(gate) * up).astype(jnp.bfloat16)
            mlp_part = jnp.dot(act, w_down[layer], preferred_element_type=jnp.float32)
            mlp_out = lax.psum_scatter(mlp_part, 'tp', scatter_dimension=0, tiled=True)
            hidden = (hidden_mid.astype(jnp.float32) + mlp_out).astype(jnp.bfloat16)
        return hidden

    return jax.shard_map(
        body,
        mesh=mesh5,
        in_specs=(row_spec, gain_spec, gain_spec, q_spec, col_spec, col_spec, o_spec, col_spec, col_spec, down_spec),
        out_specs=row_spec,
        check_vma=False,
    )
```

```python
import functools
import math
import jax
import jax.numpy as jnp
from jax import lax
from jax.experimental import pallas as pl
from jax.experimental.pallas import tpu as pltpu
from jax.sharding import Mesh, PartitionSpec as P

def seg_positions(dev_ids, rows, dev_total):
    offset = jnp.arange(rows)
    half_len = rows // 2
    seg_idx = jnp.where(offset < half_len, dev_ids[..., None], 2 * dev_total - 1 - dev_ids[..., None])
    return seg_idx * half_len + offset % half_len


SEG = 48
HD = 128
GRP = 3
XN = 4
SN = 16
RUN = XN * SEG
NRUN = 4
CH = NRUN * RUN
QR = GRP * RUN
TOK = 192
SCALE = math.log2(math.e) / math.sqrt(HD)
NB = 20


def quarter_block(quarter):
    return jnp.where(quarter == 0, 0, jnp.where(quarter == 1, 2, jnp.where(quarter == 2, 3, 1)))


def attn_kernel(q_send, kv_send, o_out, q_own, kv_all, o_own, o_recv, s_a, s_b, mx_a, mx_b, m_ref, l_ref, acc_ref,
                send_a, recv_a, send_b, recv_b, send_o, recv_o, local_sem):
    zi, yi, xi = lax.axis_index('z'), lax.axis_index('y'), lax.axis_index('x')
    group = zi * 4 + yi

    def slot(coords):
        return coords[0] * 4 + coords[1]

    def plus(v, d):
        return lax.rem(v + d + 4, 4)

    barrier = pltpu.get_barrier_semaphore()
    for d in (1, 2, 3):
        pl.semaphore_signal(barrier, inc=1, device_id={'x': plus(xi, d)}, device_id_type=pl.DeviceIdType.MESH)
    for d in (1, -1):
        pl.semaphore_signal(barrier, inc=1, device_id={'y': plus(yi, d)}, device_id_type=pl.DeviceIdType.MESH)
        pl.semaphore_signal(barrier, inc=1, device_id={'z': plus(zi, d)}, device_id_type=pl.DeviceIdType.MESH)
    own_q = pltpu.make_async_copy(q_send.at[xi], q_own.at[xi], local_sem.at[0])
    own_kv = pltpu.make_async_copy(kv_send.at[xi], kv_all.at[group, xi], local_sem.at[1])
    own_q.start()
    own_kv.start()
    pl.semaphore_wait(barrier, 7)

    def remote(src, dst, ssem, rsem, dev):
        return pltpu.make_async_remote_copy(src_ref=src, dst_ref=dst, send_sem=ssem, recv_sem=rsem, device_id=dev,
                                            device_id_type=pl.DeviceIdType.MESH)

    kv_msgs, q_msgs = [], []
    for d in (1, 2, 3):
        to = plus(xi, d)
        kv_msgs.append(remote(kv_send.at[to], kv_all.at[group, xi], send_a.at[d - 1], recv_a.at[d - 1], {'x': to}))
        q_msgs.append(remote(q_send.at[to], q_own.at[xi], send_a.at[d + 2], recv_a.at[d + 2], {'x': to}))
    for c in kv_msgs:
        c.start()
    for c in q_msgs:
        c.start()
    own_kv.wait()
    for c in kv_msgs:
        c.wait_recv()

    pos = (zi, yi)
    names = ('z', 'y')

    def at(axis, da, db):
        other = 1 - axis
        c = [None, None]
        c[axis] = plus(pos[axis], da)
        c[other] = plus(pos[other], db)
        return slot(c)

    def msg(half, idx, where, part, axis, d):
        base = half * 2
        lo, n = (base, 2) if part is None else (base + part, 1)
        ref = kv_all.at[where, pl.ds(lo, n)]
        k = half * NB + idx
        return remote(ref, ref, send_b.at[k], recv_b.at[k], {names[axis]: plus(pos[axis], d)})

    first = (1, 0)
    stage = [dict() for _ in range(2)]
    offs = (0, -1, 1, 2)

    def begin(half, key, m):
        stage[half][key] = m
        m.start()

    def send_second(half, j):
        a = first[half]
        b = 1 - a
        for s, d in enumerate((1, -1)):
            begin(half, ('b', j, d), msg(half, 4 + j * 4 + s, at(a, offs[j], 0), None, b, d))

    def forward_second(half, j):
        a = first[half]
        b = 1 - a
        for s, d in enumerate((1, -1)):
            stage[half][('b', j, d)].wait_recv()
            begin(half, ('f', j, d), msg(half, 4 + j * 4 + 2 + s, at(a, offs[j], -d), s, b, d))

    for half in range(2):
        a = first[half]
        for s, d in enumerate((1, -1)):
            begin(half, ('a', d), msg(half, s, group, None, a, d))
    for half in range(2):
        send_second(half, 0)
    for half in range(2):
        a = first[half]
        for s, d in enumerate((1, -1)):
            stage[half][('a', d)].wait_recv()
            begin(half, ('g', d), msg(half, 2 + s, at(a, -d, 0), s, a, d))
    for half in range(2):
        send_second(half, 1)
        send_second(half, 2)
    for half in range(2):
        forward_second(half, 0)
    for half in range(2):
        for d in (1, -1):
            stage[half][('g', d)].wait_recv()
        send_second(half, 3)
    for j in (1, 2, 3):
        for half in range(2):
            forward_second(half, j)
    own_q.wait()
    for c in q_msgs:
        c.wait_recv()
    for half in range(2):
        for j in range(4):
            for d in (1, -1):
                stage[half][('f', j, d)].wait_recv()

    def flash_quarter(step, carry):
        quarter = 3 - step
        blk = quarter_block(quarter)
        row0 = pl.multiple_of(blk * SEG, 16)
        desc = quarter >= 2
        order = quarter * SN + jnp.where(desc, SN - 1 - group, group)
        last = order // NRUN
        xs = [jnp.where(desc, XN - 1 - i, i) for i in range(XN)]
        qs = jnp.concatenate([q_own[x, h, pl.ds(row0, SEG), :] for h in range(GRP) for x in xs], axis=0)

        def load(c, which):
            kq = c // (SN // NRUN)
            krow = pl.multiple_of(quarter_block(kq) * SEG, 16)
            kdesc = kq >= 2
            parts = []
            for r in range(NRUN):
                idx = (c % (SN // NRUN)) * NRUN + r
                member = jnp.where(kdesc, SN - 1 - idx, idx)
                for i in range(XN):
                    x = jnp.where(kdesc, XN - 1 - i, i)
                    parts.append(kv_all[member, x, which, pl.ds(krow, SEG), :])
            return jnp.concatenate(parts, axis=0)

        def qk(c, s_ref, mx_ref, masked):
            s = lax.dot_general(qs, load(c, 0), (((1,), (1,)), ((), ())), preferred_element_type=jnp.float32)
            if masked:
                row = lax.broadcasted_iota(jnp.int32, (RUN, CH), 0)
                col = lax.broadcasted_iota(jnp.int32, (RUN, CH), 1)
                visible = col <= row + (order - c * NRUN) * RUN
                s = jnp.concatenate([jnp.where(visible, s[h * RUN:(h + 1) * RUN], -jnp.inf) for h in range(GRP)], axis=0)
            s_ref[...] = s
            mx_ref[...] = jnp.broadcast_to(jnp.max(s, axis=-1, keepdims=True), (QR, HD))

        def soft(c, s_ref, mx_ref, valid):
            vals = load(c, 1)
            for h in range(GRP):
                rows = pl.ds(h * RUN, RUN)
                m_old = m_ref[rows, :]
                mx = mx_ref[rows, :]
                if valid is not None:
                    mx = jnp.where(valid, mx, -jnp.inf)
                m_new = jnp.maximum(m_old, mx)
                alpha = jnp.exp2((m_old - m_new) * SCALE)
                bias = m_new * SCALE
                if valid is not None:
                    bias = jnp.where(valid, bias, jnp.inf)
                lsum = l_ref[rows, :] * alpha
                es = []
                for t in range(CH // HD):
                    e = jnp.exp2(s_ref[rows, t * HD:(t + 1) * HD] * SCALE - bias)
                    lsum = lsum + e
                    es.append(e.astype(jnp.bfloat16))
                pv = jnp.dot(jnp.concatenate(es, axis=1), vals, preferred_element_type=jnp.float32)
                acc_ref[rows, :] = acc_ref[rows, :] * alpha + pv
                l_ref[rows, :] = lsum
                m_ref[rows, :] = m_new

        m_ref[...] = jnp.full((QR, HD), -jnp.inf, jnp.float32)
        l_ref[...] = jnp.zeros((QR, HD), jnp.float32)
        acc_ref[...] = jnp.zeros((QR, HD), jnp.float32)
        qk(last, s_a, mx_a, True)

        def pair(p, carry):
            c_cur = jnp.where(p == 0, last, 2 * p - 1)
            c_b = jnp.minimum(2 * p, last)
            c_a = jnp.minimum(2 * p + 1, last)
            qk(c_b, s_b, mx_b, False)
            soft(c_cur, s_a, mx_a, None)
            qk(c_a, s_a, mx_a, False)
            soft(c_b, s_b, mx_b, 2 * p < last)
            return carry

        lax.fori_loop(0, (last + 2) // 2, pair, 0)
        for h in range(GRP):
            rows = pl.ds(h * RUN, RUN)
            o = (acc_ref[rows, :] / jnp.sum(l_ref[rows, :], axis=-1, keepdims=True)).astype(jnp.bfloat16)
            for i in range(XN):
                o_own[xs[i], blk, h, :, :] = o[i * SEG:(i + 1) * SEG]
        for d in (1, 2, 3):
            to = plus(xi, d)
            remote(o_own.at[to, blk], o_recv.at[xi, blk], send_o.at[step, d - 1], recv_o.at[step, d - 1], {'x': to}).start()
        return carry

    lax.fori_loop(0, 4, flash_quarter, 0)
    o_recv[xi] = o_own[xi]
    for step in range(4):
        blk = (1, 3, 2, 0)[step]
        for d in (1, 2, 3):
            to = plus(xi, d)
            c = remote(o_own.at[to, blk], o_recv.at[xi, blk], send_o.at[step, d - 1], recv_o.at[step, d - 1], {'x': to})
            c.wait_send()
            c.wait_recv()
    o_out[...] = o_recv[...]
    for c in kv_msgs + q_msgs:
        c.wait_send()
    for half in range(2):
        for c in stage[half].values():
            c.wait_send()


def attention(q_send, kv_send):
    f32 = jnp.float32
    bf16 = jnp.bfloat16
    return pl.pallas_call(
        attn_kernel,
        out_shape=jax.ShapeDtypeStruct((XN, 4, GRP, SEG, HD), bf16),
        in_specs=[pl.BlockSpec(memory_space=pltpu.HBM)] * 2,
        out_specs=pl.BlockSpec(memory_space=pltpu.VMEM),
        scratch_shapes=[
            pltpu.VMEM((XN, GRP, TOK, HD), bf16),
            pltpu.VMEM((SN, XN, 2, TOK, HD), bf16),
            pltpu.VMEM((XN, 4, GRP, SEG, HD), bf16),
            pltpu.VMEM((XN, 4, GRP, SEG, HD), bf16),
            pltpu.VMEM((QR, CH), f32),
            pltpu.VMEM((QR, CH), f32),
            pltpu.VMEM((QR, HD), f32),
            pltpu.VMEM((QR, HD), f32),
            pltpu.VMEM((QR, HD), f32),
            pltpu.VMEM((QR, HD), f32),
            pltpu.VMEM((QR, HD), f32),
            pltpu.SemaphoreType.DMA((6,)),
            pltpu.SemaphoreType.DMA((6,)),
            pltpu.SemaphoreType.DMA((2 * NB,)),
            pltpu.SemaphoreType.DMA((2 * NB,)),
            pltpu.SemaphoreType.DMA((4, 3)),
            pltpu.SemaphoreType.DMA((4, 3)),
            pltpu.SemaphoreType.DMA((2,)),
        ],
        compiler_params=pltpu.CompilerParams(vmem_limit_bytes=40 << 20, collective_id=1, has_side_effects=True),
        cost_estimate=pl.CostEstimate(flops=2 * 2 * 130 * 192 * 576 * 128, bytes_accessed=8 << 20, transcendentals=0),
        name='attn',
    )(q_send, kv_send)


D = 3072
FF = 4096
ROWS = 96
NT = 512
NO = D // NT
NG = FF // NT
NS = 10


def dense_kernel(layer, post, qkv, *refs):
    refs = list(refs)
    hidden, norms = refs.pop(0), None
    if post:
        o_in, nm_mlp, w_o, w_g, w_u, w_d = refs[:6]
        refs = refs[6:]
    if qkv:
        nm_attn, cos_ref, sin_ref, w_q, w_k, w_v = refs[:6]
        refs = refs[6:]
    if post:
        hid_out = refs.pop(0)
    if qkv:
        q_out, kv_out = refs[:2]
        refs = refs[2:]
    wbuf, wsem = refs[:2]
    refs = refs[2:]
    if post:
        o_mat, hmid, nrm1, act, acc1, snd1, rcv1, acc2, snd2, rcv2, s1, r1, s2, r2 = refs[:14]
        refs = refs[14:]
    if qkv:
        nrm2 = refs.pop(0)
    sn, rn = refs
    t_me = lax.axis_index('tp')
    sibling = {'tp': 1 - t_me}

    n_o = NO if post else 0
    g0 = n_o
    d0 = g0 + (2 * NG if post else 0)
    q0 = d0 + (NO if post else 0)
    total = q0 + (5 if qkv else 0)

    def cols(i):
        return pl.ds(pl.multiple_of(i * NT, NT), NT)

    def copies(kind, i, slot):
        sem = wsem.at[slot]
        if kind == 'o':
            return [pltpu.make_async_copy(w_o.at[layer, :, cols(i)], wbuf.at[slot, pl.ds(0, 1536)], sem)]
        if kind == 'g':
            return [pltpu.make_async_copy(w_g.at[layer, :, cols(i)], wbuf.at[slot, pl.ds(0, D)], sem)]
        if kind == 'u':
            return [pltpu.make_async_copy(w_u.at[layer, :, cols(i)], wbuf.at[slot, pl.ds(0, D)], sem)]
        if kind == 'd':
            return [pltpu.make_async_copy(w_d.at[layer, :, cols(i)], wbuf.at[slot], sem)]
        nl = layer + 1 if post else layer
        if kind == 'q':
            return [pltpu.make_async_copy(w_q.at[nl, 4 * i + h], wbuf.at[slot, pl.ds(0, D), pl.ds(h * HD, HD)], sem)
                    for h in range(4)]
        if kind == 'k':
            return [pltpu.make_async_copy(w_k.at[nl], wbuf.at[slot, pl.ds(0, D)], sem)]
        return [pltpu.make_async_copy(w_v.at[nl], wbuf.at[slot, pl.ds(0, D)], sem)]

    def issue(t):
        slot = t % NS if isinstance(t, int) else lax.rem(t, NS)

        def go(cond, kind, i):
            if isinstance(cond, bool):
                if cond:
                    for c in copies(kind, i, slot):
                        c.start()
            else:
                @pl.when(cond)
                def _():
                    for c in copies(kind, i, slot):
                        c.start()

        def both(a, b):
            return (a and b) if isinstance(a, bool) else jnp.logical_and(a, b)

        if post:
            go(t < n_o, 'o', t)
            half = (t - g0) // 2
            even = (t - g0) % 2 == 0
            inside = both(t >= g0, t < d0)
            go(both(inside, even), 'g', half)
            go(both(inside, (t - g0) % 2 == 1), 'u', half)
            go(both(t >= d0, t < q0), 'd', t - d0)
        if qkv:
            go(both(t >= q0, t < q0 + 3), 'q', t - q0)
            go(t == q0 + 3, 'k', 0)
            go(t == q0 + 4, 'v', 0)

    def wait(t, depth):
        slot = t % NS if isinstance(t, int) else lax.rem(t, NS)
        ref = wbuf.at[slot, pl.ds(0, depth)]
        pltpu.make_async_copy(ref, ref, wsem.at[slot]).wait()
        return slot

    barrier = pltpu.get_barrier_semaphore()
    pl.semaphore_signal(barrier, inc=1, device_id=sibling, device_id_type=pl.DeviceIdType.MESH)
    for t in range(min(NS, total)):
        issue(t)

    def send(src, dst, ssem, rsem):
        return pltpu.make_async_remote_copy(src_ref=src, dst_ref=dst, send_sem=ssem, recv_sem=rsem, device_id=sibling,
                                            device_id_type=pl.DeviceIdType.MESH)

    def normed(src, gain_row, nrm, idx):
        ss = jnp.zeros((ROWS, 1), jnp.float32)
        for j in range(NO):
            v = src[:, j * NT:(j + 1) * NT].astype(jnp.float32)
            ss = ss + jnp.sum(v * v, axis=-1, keepdims=True)
        inv = lax.rsqrt(ss / D + 1e-5)
        for j in range(NO):
            sl = slice(j * NT, (j + 1) * NT)
            nrm[0:ROWS, sl] = (src[:, sl].astype(jnp.float32) * inv * gain_row[:, sl]).astype(jnp.bfloat16)
        c = send(nrm.at[pl.ds(0, ROWS)], nrm.at[pl.ds(ROWS, ROWS)], sn.at[idx], rn.at[idx])
        c.start()
        return c

    def part_copy(snd, rcv, ss, rs, i):
        return send(snd.at[i], rcv.at[i], ss.at[i], rs.at[i])

    def residual(base, acc, rcv, out, snd, ss, rs):
        for j in range(NO):
            part_copy(snd, rcv, ss, rs, j).wait_recv()
            sl = slice(j * NT, (j + 1) * NT)
            out[:, sl] = (base[:, sl].astype(jnp.float32) + (acc[j] + rcv[j])).astype(jnp.bfloat16)

    pending = []
    if post:
        for blk in range(4):
            row = pl.multiple_of(jnp.where(t_me == blk // 2, 0, ROWS) + (blk % 2) * SEG, 16)
            for x in range(XN):
                for h in range(GRP):
                    c0 = (x * GRP + h) * HD
                    o_mat[pl.ds(row, SEG), c0:c0 + HD] = o_in[x, blk, h]
        pl.semaphore_wait(barrier, 1)

        def o_step(i, carry):
            slot = wait(i, 1536)
            p = jnp.dot(o_mat[...], wbuf[slot, pl.ds(0, 1536), :], preferred_element_type=jnp.float32)
            acc1[i] = p[:ROWS]
            snd1[i] = p[ROWS:]
            part_copy(snd1, rcv1, s1, r1, i).start()
            issue(i + NS)
            return carry

        lax.fori_loop(0, NO, o_step, 0)
        residual(hidden, acc1, rcv1, hmid, snd1, s1, r1)
        c = normed(hmid, nm_mlp[...].astype(jnp.float32)[layer:layer + 1], nrm1, 0)
        c.wait_recv()
        pending.append(c)

        def g_step(i, carry):
            t = g0 + 2 * i
            slot_g = wait(t, D)
            g = jnp.dot(nrm1[...], wbuf[slot_g, pl.ds(0, D), :], preferred_element_type=jnp.float32)
            issue(t + NS)
            slot_u = wait(t + 1, D)
            u = jnp.dot(nrm1[...], wbuf[slot_u, pl.ds(0, D), :], preferred_element_type=jnp.float32)
            act[:, cols(i)] = (g * lax.logistic(g) * u).astype(jnp.bfloat16)
            issue(t + 1 + NS)
            return carry

        lax.fori_loop(0, NG, g_step, 0)

        def d_step(i, carry):
            slot = wait(d0 + i, FF)
            p = jnp.dot(act[...], wbuf[slot], preferred_element_type=jnp.float32)
            acc2[i] = p[:ROWS]
            snd2[i] = p[ROWS:]
            part_copy(snd2, rcv2, s2, r2, i).start()
            issue(d0 + i + NS)
            return carry

        lax.fori_loop(0, NO, d_step, 0)
        residual(hmid, acc2, rcv2, hid_out, snd2, s2, r2)
        cur = hid_out
    else:
        pl.semaphore_wait(barrier, 1)
        cur = hidden
    if qkv:
        nl = layer + 1 if post else layer
        c = normed(cur, nm_attn[...].astype(jnp.float32)[nl:nl + 1], nrm2, 1)
        c.wait_recv()
        pending.append(c)
        mine = pl.ds(pl.multiple_of(t_me * ROWS, 16), ROWS)
        theirs = pl.ds(pl.multiple_of((1 - t_me) * ROWS, 16), ROWS)

        def project(t):
            slot = wait(t, D)
            return jnp.dot(nrm2[...], wbuf[slot, pl.ds(0, D), :], preferred_element_type=jnp.float32)

        def rotate(v):
            return v * cos_ref[...] + pltpu.roll(v, HD // 2, 1) * sin_ref[...]

        def q_step(i, carry):
            p = project(q0 + i)
            for h in range(4):
                r = rotate(p[:, h * HD:(h + 1) * HD]).astype(jnp.bfloat16)
                q_out[4 * i + h, mine, :] = r[:ROWS]
                q_out[4 * i + h, theirs, :] = r[ROWS:]
            return carry

        lax.fori_loop(0, 3, q_step, 0)
        for which in range(2):
            p = project(q0 + 3 + which)
            for h in range(4):
                r = p[:, h * HD:(h + 1) * HD]
                r = (rotate(r) if which == 0 else r).astype(jnp.bfloat16)
                kv_out[h, which, mine, :] = r[:ROWS]
                kv_out[h, which, theirs, :] = r[ROWS:]
    for c in pending:
        c.wait_send()
    if post:
        for i in range(NO):
            part_copy(snd1, rcv1, s1, r1, i).wait_send()
            part_copy(snd2, rcv2, s2, r2, i).wait_send()


def dense(layer, post, qkv, hidden, o=None, norm_mlp=None, w_o=None, w_g=None, w_u=None, w_d=None, norm_attn=None, cos_t=None,
          sin_t=None, w_q=None, w_k=None, w_v=None):
    f32, bf16 = jnp.float32, jnp.bfloat16
    vmem = pl.BlockSpec(memory_space=pltpu.VMEM)
    hbm = pl.BlockSpec(memory_space=pltpu.HBM)
    args, specs, outs, scratch = [hidden], [vmem], [], []
    if post:
        args += [o, norm_mlp, w_o, w_g, w_u, w_d]
        specs += [vmem, vmem] + [hbm] * 4
        outs.append(jax.ShapeDtypeStruct((ROWS, D), bf16))
    if qkv:
        args += [norm_attn, cos_t, sin_t, w_q, w_k, w_v]
        specs += [vmem] * 3 + [hbm] * 3
        outs += [jax.ShapeDtypeStruct((XN * GRP, TOK, HD), bf16), jax.ShapeDtypeStruct((XN, 2, TOK, HD), bf16)]
    scratch += [pltpu.VMEM((NS, FF, NT), bf16), pltpu.SemaphoreType.DMA((NS,))]
    if post:
        part = pltpu.VMEM((NO, ROWS, NT), f32)
        scratch += [pltpu.VMEM((TOK, 1536), bf16), pltpu.VMEM((ROWS, D), bf16), pltpu.VMEM((TOK, D), bf16),
                    pltpu.VMEM((TOK, FF), bf16)] + [part] * 6 + [pltpu.SemaphoreType.DMA((NO,))] * 4
    if qkv:
        scratch += [pltpu.VMEM((TOK, D), bf16)]
    scratch += [pltpu.SemaphoreType.DMA((2,))] * 2
    moved = (85 << 20 if post else 0) + (16 << 20 if qkv else 0)
    return pl.pallas_call(
        functools.partial(dense_kernel, layer, post, qkv),
        out_shape=tuple(outs),
        in_specs=specs,
        out_specs=tuple([vmem] * len(outs)),
        scratch_shapes=scratch,
        compiler_params=pltpu.CompilerParams(vmem_limit_bytes=63 << 20, collective_id=2 + layer + (1 if post else 0),
                                             has_side_effects=True),
        cost_estimate=pl.CostEstimate(flops=TOK * moved, bytes_accessed=moved, transcendentals=0),
        name=f'dense{layer}{int(post)}{int(qkv)}',
    )(*args)


def solution(mesh):
    tp_size = mesh.shape['tp']
    cp_size = mesh.shape['cp']
    dev_total = tp_size * cp_size
    mesh5 = Mesh(mesh.devices.reshape(1, tp_size, 4, 4, 4), ('dp', 'tp', 'z', 'y', 'x'))
    row_spec = P(('dp', 'tp', 'z', 'y', 'x'), None)
    gain_spec = P(None, None)
    q_spec = P(None, None, 'tp', None)
    col_spec = P(None, None, 'tp')
    o_spec = P(None, 'tp', None, None)
    down_spec = P(None, 'tp', None)

    def body(tokens, norm_attn, norm_mlp, w_q, w_k, w_v, w_o, w_gate, w_up, w_down):
        rows = tokens.shape[0]
        tp_idx = lax.axis_index('tp')
        cp_idx = (lax.axis_index('z') * 4 + lax.axis_index('y')) * 4 + lax.axis_index('x')
        tp_devs = jnp.stack([tp_idx, 1 - tp_idx]) * cp_size + cp_idx
        pos = seg_positions(tp_devs, rows, dev_total).reshape(tp_size * rows)
        inv_freq = 500000.0 ** (-(jnp.arange(HD // 2, dtype=jnp.float32) * 2.0 / HD))
        angles = pos.astype(jnp.float32)[:, None] * inv_freq[None, :]
        cos_a, sin_a = jnp.cos(angles), jnp.sin(angles)
        cos_t = jnp.concatenate([cos_a, cos_a], axis=1)
        sin_t = jnp.concatenate([-sin_a, sin_a], axis=1)
        layers = w_q.shape[0]
        proj = dict(norm_attn=norm_attn, cos_t=cos_t, sin_t=sin_t, w_q=w_q.transpose(0, 2, 1, 3), w_k=w_k, w_v=w_v)
        ffn = dict(norm_mlp=norm_mlp, w_o=w_o.reshape(layers, -1, D), w_g=w_gate, w_u=w_up, w_d=w_down)
        hidden = tokens
        q_send, kv_send = dense(0, False, True, hidden, **proj)
        for layer in range(layers):
            o = attention(q_send.reshape(XN, GRP, TOK, HD), kv_send)
            if layer + 1 < layers:
                hidden, q_send, kv_send = dense(layer, True, True, hidden, o=o, **ffn, **proj)
            else:
                hidden, = dense(layer, True, False, hidden, o=o, **ffn)
        return hidden

    return jax.shard_map(
        body,
        mesh=mesh5,
        in_specs=(row_spec, gain_spec, gain_spec, q_spec, col_spec, col_spec, o_spec, col_spec, col_spec, down_spec),
        out_specs=row_spec,
        check_vma=False,
    )
```

```python
import functools
import math
import jax
import jax.numpy as jnp
from jax import lax
from jax.experimental import pallas as pl
from jax.experimental.pallas import tpu as pltpu
from jax.sharding import Mesh, PartitionSpec as P

def seg_positions(dev_ids, rows, dev_total):
    offset = jnp.arange(rows)
    half_len = rows // 2
    seg_idx = jnp.where(offset < half_len, dev_ids[..., None], 2 * dev_total - 1 - dev_ids[..., None])
    return seg_idx * half_len + offset % half_len


SEG = 48
HD = 128
GRP = 3
XN = 4
SN = 16
RUN = XN * SEG
NRUN = 4
CH = NRUN * RUN
QR = GRP * RUN
TOK = 192
SCALE = math.log2(math.e) / math.sqrt(HD)
NB = 20
STRIP = 64


def quarter_block(quarter):
    return jnp.where(quarter == 0, 0, jnp.where(quarter == 1, 2, jnp.where(quarter == 2, 3, 1)))


def attn_kernel(q_send, kv_send, o_out, q_own, kv_all, o_own, o_recv, s_a, s_b, mx_a, mx_b, e_buf, m_ref, l_ref, acc_ref,
                send_a, recv_a, send_b, recv_b, send_o, recv_o, local_sem):
    zi, yi, xi = lax.axis_index('z'), lax.axis_index('y'), lax.axis_index('x')
    group = zi * 4 + yi

    def slot(coords):
        return coords[0] * 4 + coords[1]

    def plus(v, d):
        return lax.rem(v + d + 4, 4)

    barrier = pltpu.get_barrier_semaphore()
    for d in (1, 2, 3):
        pl.semaphore_signal(barrier, inc=1, device_id={'x': plus(xi, d)}, device_id_type=pl.DeviceIdType.MESH)
    for d in (1, -1):
        pl.semaphore_signal(barrier, inc=1, device_id={'y': plus(yi, d)}, device_id_type=pl.DeviceIdType.MESH)
        pl.semaphore_signal(barrier, inc=1, device_id={'z': plus(zi, d)}, device_id_type=pl.DeviceIdType.MESH)
    own_q = pltpu.make_async_copy(q_send.at[xi], q_own.at[xi], local_sem.at[0])
    own_kv = pltpu.make_async_copy(kv_send.at[xi], kv_all.at[group, xi], local_sem.at[1])
    own_q.start()
    own_kv.start()
    pl.semaphore_wait(barrier, 7)

    def remote(src, dst, ssem, rsem, dev):
        return pltpu.make_async_remote_copy(src_ref=src, dst_ref=dst, send_sem=ssem, recv_sem=rsem, device_id=dev,
                                            device_id_type=pl.DeviceIdType.MESH)

    kv_msgs, q_msgs = [], []
    for d in (1, 2, 3):
        to = plus(xi, d)
        kv_msgs.append(remote(kv_send.at[to], kv_all.at[group, xi], send_a.at[d - 1], recv_a.at[d - 1], {'x': to}))
        q_msgs.append(remote(q_send.at[to], q_own.at[xi], send_a.at[d + 2], recv_a.at[d + 2], {'x': to}))
    for c in kv_msgs:
        c.start()
    for c in q_msgs:
        c.start()
    own_kv.wait()
    for c in kv_msgs:
        c.wait_recv()

    pos = (zi, yi)
    names = ('z', 'y')

    def at(axis, da, db):
        other = 1 - axis
        c = [None, None]
        c[axis] = plus(pos[axis], da)
        c[other] = plus(pos[other], db)
        return slot(c)

    def msg(half, idx, where, part, axis, d):
        base = half * 2
        lo, n = (base, 2) if part is None else (base + part, 1)
        ref = kv_all.at[where, pl.ds(lo, n)]
        k = half * NB + idx
        return remote(ref, ref, send_b.at[k], recv_b.at[k], {names[axis]: plus(pos[axis], d)})

    first = (1, 0)
    stage = [dict() for _ in range(2)]
    offs = (0, -1, 1, 2)

    def begin(half, key, m):
        stage[half][key] = m
        m.start()

    def send_second(half, j):
        a = first[half]
        b = 1 - a
        for s, d in enumerate((1, -1)):
            begin(half, ('b', j, d), msg(half, 4 + j * 4 + s, at(a, offs[j], 0), None, b, d))

    def forward_second(half, j):
        a = first[half]
        b = 1 - a
        for s, d in enumerate((1, -1)):
            stage[half][('b', j, d)].wait_recv()
            begin(half, ('f', j, d), msg(half, 4 + j * 4 + 2 + s, at(a, offs[j], -d), s, b, d))

    Y, Z = 0, 1

    def send_first(half):
        for s, d in enumerate((1, -1)):
            begin(half, ('a', d), msg(half, s, group, None, first[half], d))

    def forward_first(half):
        a = first[half]
        for s, d in enumerate((1, -1)):
            begin(half, ('g', d), msg(half, 2 + s, at(a, -d, 0), s, a, d))

    def got(half, *key):
        for d in (1, -1):
            stage[half][key + (d,)].wait_recv()

    def quarter_rows(t):
        desc = t >= 2
        return quarter_block(t), desc, [jnp.where(desc, XN - 1 - i, i) for i in range(XN)]

    def load_q(t):
        blk, _, xs = quarter_rows(t)
        row0 = pl.multiple_of(blk * SEG, 16)
        return jnp.concatenate([q_own[x, h, pl.ds(row0, SEG), :] for h in range(GRP) for x in xs], axis=0)

    def load_kv(kq, zr, which):
        blk, desc, xs = quarter_rows(kq)
        krow = pl.multiple_of(blk * SEG, 16)
        parts = []
        for r in range(NRUN):
            member = zr * 4 + jnp.where(desc, NRUN - 1 - r, r)
            for x in xs:
                parts.append(kv_all[member, x, which, pl.ds(krow, SEG), :])
        return jnp.concatenate(parts, axis=0)

    def entry(e, lower, own):
        n0 = 4 if own else 2
        u = e - n0
        t = 1 + jnp.where(u >= 1, 1, 0) + jnp.where(u >= 3, 1, 0)
        kq = jnp.where(u < 1, 0, jnp.where(u < 3, u - 1, u - 3))
        t0 = e if own else jnp.where(lower, e, e + 2)
        return jnp.where(u < 0, t0, t), jnp.where(u < 0, t0, kq)

    def qk(tk, zr, s_ref, mx_ref, own):
        t, kq = tk
        s = lax.dot_general(load_q(t), load_kv(kq, zr, 0), (((1,), (1,)), ((), ())), preferred_element_type=jnp.float32)
        if own:
            row = lax.broadcasted_iota(jnp.int32, (RUN, CH), 0)
            col = lax.broadcasted_iota(jnp.int32, (RUN, CH), 1)
            mine = jnp.where(t >= 2, NRUN - 1 - yi, yi) * RUN
            visible = col <= row + jnp.where(t == kq, mine, CH)
            s = jnp.concatenate([jnp.where(visible, s[h * RUN:(h + 1) * RUN], -jnp.inf) for h in range(GRP)], axis=0)
        s_ref[...] = s
        mx_ref[...] = jnp.broadcast_to(jnp.max(s, axis=-1, keepdims=True), (QR, HD))

    def soft(tk, zr, s_ref, mx_ref):
        t, kq = tk
        vals = load_kv(kq, zr, 1)
        for h in range(GRP):
            for r0 in range(h * RUN, (h + 1) * RUN, STRIP):
                rows = slice(r0, r0 + STRIP)
                m_old = m_ref[t, rows, :]
                m_new = jnp.maximum(m_old, mx_ref[rows, :])
                alpha = jnp.exp2((m_old - m_new) * SCALE)
                bias = m_new * SCALE
                lsum = l_ref[t, rows, :] * alpha
                for c in range(CH // HD):
                    e = jnp.exp2(s_ref[rows, c * HD:(c + 1) * HD] * SCALE - bias)
                    lsum = lsum + e
                    e_buf[rows, c * HD:(c + 1) * HD] = e.astype(jnp.bfloat16)
                m_ref[t, rows, :] = m_new
                l_ref[t, rows, :] = lsum
                acc_ref[t, rows, :] = acc_ref[t, rows, :] * alpha
            rows = slice(h * RUN, (h + 1) * RUN)
            acc_ref[t, rows, :] += jnp.dot(e_buf[rows, :], vals, preferred_element_type=jnp.float32)

    def run_row(zr, lower, own, lo, hi, after=None):
        n = 10 if own else 8
        if lo == 0:
            qk(entry(0, lower, own), zr, s_a, mx_a, own)

        def pair(p, carry):
            qk(entry(2 * p + 1, lower, own), zr, s_b, mx_b, own)
            soft(entry(2 * p, lower, own), zr, s_a, mx_a)
            qk(entry(jnp.minimum(2 * p + 2, n - 1), lower, own), zr, s_a, mx_a, own)
            soft(entry(2 * p + 1, lower, own), zr, s_b, mx_b)
            if after is not None:
                after(p)
            return carry

        lax.fori_loop(lo, hi, pair, 0)

    def o_msg(step, d):
        to = plus(xi, d)
        blk = quarter_block(step)
        return remote(o_own.at[to, blk], o_recv.at[xi, blk], send_o.at[step, d - 1], recv_o.at[step, d - 1], {'x': to})

    def finish(t):
        blk, _, xs = quarter_rows(t)
        for h in range(GRP):
            rows = slice(h * RUN, (h + 1) * RUN)
            o = (acc_ref[t, rows, :] / jnp.sum(l_ref[t, rows, :], axis=-1, keepdims=True)).astype(jnp.bfloat16)
            for i in range(XN):
                o_own[xs[i], blk, h, :, :] = o[i * SEG:(i + 1) * SEG]
        for d in (2, 1, 3):
            o_msg(t, d).start()

    send_first(Y)
    send_second(Y, 0)
    send_second(Z, 0)
    send_first(Z)
    m_ref[...] = jnp.full((4, QR, HD), -jnp.inf, jnp.float32)
    l_ref[...] = jnp.zeros((4, QR, HD), jnp.float32)
    acc_ref[...] = jnp.zeros((4, QR, HD), jnp.float32)
    got(Y, 'a')
    forward_first(Y)
    send_second(Y, 1)
    send_second(Y, 2)
    forward_second(Z, 0)
    got(Z, 'a')
    send_second(Z, 1)
    send_second(Z, 2)
    got(Y, 'g')
    send_second(Y, 3)
    forward_second(Y, 0)
    forward_first(Z)
    own_q.wait()
    for c in q_msgs:
        c.wait_recv()
    got(Z, 'f', 0)
    rows_z = [plus(zi, d) for d in offs]
    lower = [r < zi for r in rows_z]
    run_row(zi, None, True, 0, 3)
    forward_second(Z, 1)
    forward_second(Y, 1)
    run_row(zi, None, True, 3, 5)
    forward_second(Z, 2)
    forward_second(Y, 2)
    got(Z, 'g')
    send_second(Z, 3)
    forward_second(Y, 3)
    got(Z, 'f', 1)
    run_row(rows_z[1], lower[1], False, 0, 4)
    forward_second(Z, 3)
    got(Z, 'f', 2)
    run_row(rows_z[2], lower[2], False, 0, 4)
    for j in range(4):
        got(Y, 'f', j)
    got(Z, 'f', 3)
    run_row(rows_z[3], lower[3], False, 0, 4, after=finish)
    o_recv[xi] = o_own[xi]
    for step in range(4):
        for d in (1, 2, 3):
            c = o_msg(step, d)
            c.wait_send()
            c.wait_recv()
    o_out[...] = o_recv[...]
    for c in kv_msgs + q_msgs:
        c.wait_send()
    for half in range(2):
        for c in stage[half].values():
            c.wait_send()


def attention(q_send, kv_send):
    f32 = jnp.float32
    bf16 = jnp.bfloat16
    return pl.pallas_call(
        attn_kernel,
        out_shape=jax.ShapeDtypeStruct((XN, 4, GRP, SEG, HD), bf16),
        in_specs=[pl.BlockSpec(memory_space=pltpu.HBM)] * 2,
        out_specs=pl.BlockSpec(memory_space=pltpu.VMEM),
        scratch_shapes=[
            pltpu.VMEM((XN, GRP, TOK, HD), bf16),
            pltpu.VMEM((SN, XN, 2, TOK, HD), bf16),
            pltpu.VMEM((XN, 4, GRP, SEG, HD), bf16),
            pltpu.VMEM((XN, 4, GRP, SEG, HD), bf16),
            pltpu.VMEM((QR, CH), f32),
            pltpu.VMEM((QR, CH), f32),
            pltpu.VMEM((QR, HD), f32),
            pltpu.VMEM((QR, HD), f32),
            pltpu.VMEM((QR, CH), bf16),
            pltpu.VMEM((4, QR, HD), f32),
            pltpu.VMEM((4, QR, HD), f32),
            pltpu.VMEM((4, QR, HD), f32),
            pltpu.SemaphoreType.DMA((6,)),
            pltpu.SemaphoreType.DMA((6,)),
            pltpu.SemaphoreType.DMA((2 * NB,)),
            pltpu.SemaphoreType.DMA((2 * NB,)),
            pltpu.SemaphoreType.DMA((4, 3)),
            pltpu.SemaphoreType.DMA((4, 3)),
            pltpu.SemaphoreType.DMA((2,)),
        ],
        compiler_params=pltpu.CompilerParams(vmem_limit_bytes=40 << 20, collective_id=1, has_side_effects=True),
        cost_estimate=pl.CostEstimate(flops=2 * 2 * 130 * 192 * 576 * 128, bytes_accessed=8 << 20, transcendentals=0),
        name='attn',
    )(q_send, kv_send)


D = 3072
FF = 4096
ROWS = 96
NT = 512
NO = D // NT
NG = FF // NT
NS = 10


def dense_kernel(layer, post, qkv, *refs):
    refs = list(refs)
    hidden, norms = refs.pop(0), None
    if post:
        o_in, nm_mlp, w_o, w_g, w_u, w_d = refs[:6]
        refs = refs[6:]
    if qkv:
        nm_attn, cos_ref, sin_ref, w_q, w_k, w_v = refs[:6]
        refs = refs[6:]
    if post:
        hid_out = refs.pop(0)
    if qkv:
        q_out, kv_out = refs[:2]
        refs = refs[2:]
    wbuf, wsem = refs[:2]
    refs = refs[2:]
    if post:
        o_mat, hmid, nrm1, act, acc1, snd1, rcv1, acc2, snd2, rcv2, s1, r1, s2, r2 = refs[:14]
        refs = refs[14:]
    if qkv:
        nrm2 = refs.pop(0)
    sn, rn = refs
    t_me = lax.axis_index('tp')
    sibling = {'tp': 1 - t_me}

    n_o = NO if post else 0
    g0 = n_o
    d0 = g0 + (2 * NG if post else 0)
    q0 = d0 + (NO if post else 0)
    total = q0 + (5 if qkv else 0)

    def cols(i):
        return pl.ds(pl.multiple_of(i * NT, NT), NT)

    def copies(kind, i, slot):
        sem = wsem.at[slot]
        if kind == 'o':
            return [pltpu.make_async_copy(w_o.at[layer, :, cols(i)], wbuf.at[slot, pl.ds(0, 1536)], sem)]
        if kind == 'g':
            return [pltpu.make_async_copy(w_g.at[layer, :, cols(i)], wbuf.at[slot, pl.ds(0, D)], sem)]
        if kind == 'u':
            return [pltpu.make_async_copy(w_u.at[layer, :, cols(i)], wbuf.at[slot, pl.ds(0, D)], sem)]
        if kind == 'd':
            return [pltpu.make_async_copy(w_d.at[layer, :, cols(i)], wbuf.at[slot], sem)]
        nl = layer + 1 if post else layer
        if kind == 'q':
            return [pltpu.make_async_copy(w_q.at[nl, 4 * i + h], wbuf.at[slot, pl.ds(0, D), pl.ds(h * HD, HD)], sem)
                    for h in range(4)]
        if kind == 'k':
            return [pltpu.make_async_copy(w_k.at[nl], wbuf.at[slot, pl.ds(0, D)], sem)]
        return [pltpu.make_async_copy(w_v.at[nl], wbuf.at[slot, pl.ds(0, D)], sem)]

    def issue(t):
        slot = t % NS if isinstance(t, int) else lax.rem(t, NS)

        def go(cond, kind, i):
            if isinstance(cond, bool):
                if cond:
                    for c in copies(kind, i, slot):
                        c.start()
            else:
                @pl.when(cond)
                def _():
                    for c in copies(kind, i, slot):
                        c.start()

        def both(a, b):
            return (a and b) if isinstance(a, bool) else jnp.logical_and(a, b)

        if post:
            go(t < n_o, 'o', t)
            half = (t - g0) // 2
            even = (t - g0) % 2 == 0
            inside = both(t >= g0, t < d0)
            go(both(inside, even), 'g', half)
            go(both(inside, (t - g0) % 2 == 1), 'u', half)
            go(both(t >= d0, t < q0), 'd', t - d0)
        if qkv:
            go(both(t >= q0, t < q0 + 3), 'q', t - q0)
            go(t == q0 + 3, 'k', 0)
            go(t == q0 + 4, 'v', 0)

    def wait(t, depth):
        slot = t % NS if isinstance(t, int) else lax.rem(t, NS)
        ref = wbuf.at[slot, pl.ds(0, depth)]
        pltpu.make_async_copy(ref, ref, wsem.at[slot]).wait()
        return slot

    barrier = pltpu.get_barrier_semaphore()
    pl.semaphore_signal(barrier, inc=1, device_id=sibling, device_id_type=pl.DeviceIdType.MESH)
    for t in range(min(NS, total)):
        issue(t)

    def send(src, dst, ssem, rsem):
        return pltpu.make_async_remote_copy(src_ref=src, dst_ref=dst, send_sem=ssem, recv_sem=rsem, device_id=sibling,
                                            device_id_type=pl.DeviceIdType.MESH)

    def normed(src, gain_row, nrm, idx):
        ss = jnp.zeros((ROWS, 1), jnp.float32)
        for j in range(NO):
            v = src[:, j * NT:(j + 1) * NT].astype(jnp.float32)
            ss = ss + jnp.sum(v * v, axis=-1, keepdims=True)
        inv = lax.rsqrt(ss / D + 1e-5)
        for j in range(NO):
            sl = slice(j * NT, (j + 1) * NT)
            nrm[0:ROWS, sl] = (src[:, sl].astype(jnp.float32) * inv * gain_row[:, sl]).astype(jnp.bfloat16)
        c = send(nrm.at[pl.ds(0, ROWS)], nrm.at[pl.ds(ROWS, ROWS)], sn.at[idx], rn.at[idx])
        c.start()
        return c

    def part_copy(snd, rcv, ss, rs, i):
        return send(snd.at[i], rcv.at[i], ss.at[i], rs.at[i])

    def residual(base, acc, rcv, out, snd, ss, rs):
        for j in range(NO):
            part_copy(snd, rcv, ss, rs, j).wait_recv()
            sl = slice(j * NT, (j + 1) * NT)
            out[:, sl] = (base[:, sl].astype(jnp.float32) + (acc[j] + rcv[j])).astype(jnp.bfloat16)

    pending = []
    if post:
        for blk in range(4):
            row = pl.multiple_of(jnp.where(t_me == blk // 2, 0, ROWS) + (blk % 2) * SEG, 16)
            for x in range(XN):
                for h in range(GRP):
                    c0 = (x * GRP + h) * HD
                    o_mat[pl.ds(row, SEG), c0:c0 + HD] = o_in[x, blk, h]
        pl.semaphore_wait(barrier, 1)

        def o_step(i, carry):
            slot = wait(i, 1536)
            p = jnp.dot(o_mat[...], wbuf[slot, pl.ds(0, 1536), :], preferred_element_type=jnp.float32)
            acc1[i] = p[:ROWS]
            snd1[i] = p[ROWS:]
            part_copy(snd1, rcv1, s1, r1, i).start()
            issue(i + NS)
            return carry

        lax.fori_loop(0, NO, o_step, 0)
        residual(hidden, acc1, rcv1, hmid, snd1, s1, r1)
        c = normed(hmid, nm_mlp[...].astype(jnp.float32)[layer:layer + 1], nrm1, 0)
        c.wait_recv()
        pending.append(c)

        def g_step(i, carry):
            t = g0 + 2 * i
            slot_g = wait(t, D)
            g = jnp.dot(nrm1[...], wbuf[slot_g, pl.ds(0, D), :], preferred_element_type=jnp.float32)
            issue(t + NS)
            slot_u = wait(t + 1, D)
            u = jnp.dot(nrm1[...], wbuf[slot_u, pl.ds(0, D), :], preferred_element_type=jnp.float32)
            act[:, cols(i)] = (g * lax.logistic(g) * u).astype(jnp.bfloat16)
            issue(t + 1 + NS)
            return carry

        lax.fori_loop(0, NG, g_step, 0)

        def d_step(i, carry):
            slot = wait(d0 + i, FF)
            p = jnp.dot(act[...], wbuf[slot], preferred_element_type=jnp.float32)
            acc2[i] = p[:ROWS]
            snd2[i] = p[ROWS:]
            part_copy(snd2, rcv2, s2, r2, i).start()
            issue(d0 + i + NS)
            return carry

        lax.fori_loop(0, NO, d_step, 0)
        residual(hmid, acc2, rcv2, hid_out, snd2, s2, r2)
        cur = hid_out
    else:
        pl.semaphore_wait(barrier, 1)
        cur = hidden
    if qkv:
        nl = layer + 1 if post else layer
        c = normed(cur, nm_attn[...].astype(jnp.float32)[nl:nl + 1], nrm2, 1)
        c.wait_recv()
        pending.append(c)
        mine = pl.ds(pl.multiple_of(t_me * ROWS, 16), ROWS)
        theirs = pl.ds(pl.multiple_of((1 - t_me) * ROWS, 16), ROWS)

        def project(t):
            slot = wait(t, D)
            return jnp.dot(nrm2[...], wbuf[slot, pl.ds(0, D), :], preferred_element_type=jnp.float32)

        def rotate(v):
            return v * cos_ref[...] + pltpu.roll(v, HD // 2, 1) * sin_ref[...]

        def q_step(i, carry):
            p = project(q0 + i)
            for h in range(4):
                r = rotate(p[:, h * HD:(h + 1) * HD]).astype(jnp.bfloat16)
                q_out[4 * i + h, mine, :] = r[:ROWS]
                q_out[4 * i + h, theirs, :] = r[ROWS:]
            return carry

        lax.fori_loop(0, 3, q_step, 0)
        for which in range(2):
            p = project(q0 + 3 + which)
            for h in range(4):
                r = p[:, h * HD:(h + 1) * HD]
                r = (rotate(r) if which == 0 else r).astype(jnp.bfloat16)
                kv_out[h, which, mine, :] = r[:ROWS]
                kv_out[h, which, theirs, :] = r[ROWS:]
    for c in pending:
        c.wait_send()
    if post:
        for i in range(NO):
            part_copy(snd1, rcv1, s1, r1, i).wait_send()
            part_copy(snd2, rcv2, s2, r2, i).wait_send()


def dense(layer, post, qkv, hidden, o=None, norm_mlp=None, w_o=None, w_g=None, w_u=None, w_d=None, norm_attn=None, cos_t=None,
          sin_t=None, w_q=None, w_k=None, w_v=None):
    f32, bf16 = jnp.float32, jnp.bfloat16
    vmem = pl.BlockSpec(memory_space=pltpu.VMEM)
    hbm = pl.BlockSpec(memory_space=pltpu.HBM)
    args, specs, outs, scratch = [hidden], [vmem], [], []
    if post:
        args += [o, norm_mlp, w_o, w_g, w_u, w_d]
        specs += [vmem, vmem] + [hbm] * 4
        outs.append(jax.ShapeDtypeStruct((ROWS, D), bf16))
    if qkv:
        args += [norm_attn, cos_t, sin_t, w_q, w_k, w_v]
        specs += [vmem] * 3 + [hbm] * 3
        outs += [jax.ShapeDtypeStruct((XN * GRP, TOK, HD), bf16), jax.ShapeDtypeStruct((XN, 2, TOK, HD), bf16)]
    scratch += [pltpu.VMEM((NS, FF, NT), bf16), pltpu.SemaphoreType.DMA((NS,))]
    if post:
        part = pltpu.VMEM((NO, ROWS, NT), f32)
        scratch += [pltpu.VMEM((TOK, 1536), bf16), pltpu.VMEM((ROWS, D), bf16), pltpu.VMEM((TOK, D), bf16),
                    pltpu.VMEM((TOK, FF), bf16)] + [part] * 6 + [pltpu.SemaphoreType.DMA((NO,))] * 4
    if qkv:
        scratch += [pltpu.VMEM((TOK, D), bf16)]
    scratch += [pltpu.SemaphoreType.DMA((2,))] * 2
    moved = (85 << 20 if post else 0) + (16 << 20 if qkv else 0)
    return pl.pallas_call(
        functools.partial(dense_kernel, layer, post, qkv),
        out_shape=tuple(outs),
        in_specs=specs,
        out_specs=tuple([vmem] * len(outs)),
        scratch_shapes=scratch,
        compiler_params=pltpu.CompilerParams(vmem_limit_bytes=63 << 20, collective_id=2 + layer + (1 if post else 0),
                                             has_side_effects=True),
        cost_estimate=pl.CostEstimate(flops=TOK * moved, bytes_accessed=moved, transcendentals=0),
        name=f'dense{layer}{int(post)}{int(qkv)}',
    )(*args)


def solution(mesh):
    tp_size = mesh.shape['tp']
    cp_size = mesh.shape['cp']
    dev_total = tp_size * cp_size
    mesh5 = Mesh(mesh.devices.reshape(1, tp_size, 4, 4, 4), ('dp', 'tp', 'z', 'y', 'x'))
    row_spec = P(('dp', 'tp', 'z', 'y', 'x'), None)
    gain_spec = P(None, None)
    q_spec = P(None, None, 'tp', None)
    col_spec = P(None, None, 'tp')
    o_spec = P(None, 'tp', None, None)
    down_spec = P(None, 'tp', None)

    def body(tokens, norm_attn, norm_mlp, w_q, w_k, w_v, w_o, w_gate, w_up, w_down):
        rows = tokens.shape[0]
        tp_idx = lax.axis_index('tp')
        cp_idx = (lax.axis_index('z') * 4 + lax.axis_index('y')) * 4 + lax.axis_index('x')
        tp_devs = jnp.stack([tp_idx, 1 - tp_idx]) * cp_size + cp_idx
        pos = seg_positions(tp_devs, rows, dev_total).reshape(tp_size * rows)
        inv_freq = 500000.0 ** (-(jnp.arange(HD // 2, dtype=jnp.float32) * 2.0 / HD))
        angles = pos.astype(jnp.float32)[:, None] * inv_freq[None, :]
        cos_a, sin_a = jnp.cos(angles), jnp.sin(angles)
        cos_t = jnp.concatenate([cos_a, cos_a], axis=1)
        sin_t = jnp.concatenate([-sin_a, sin_a], axis=1)
        layers = w_q.shape[0]
        proj = dict(norm_attn=norm_attn, cos_t=cos_t, sin_t=sin_t, w_q=w_q.transpose(0, 2, 1, 3), w_k=w_k, w_v=w_v)
        ffn = dict(norm_mlp=norm_mlp, w_o=w_o.reshape(layers, -1, D), w_g=w_gate, w_u=w_up, w_d=w_down)
        hidden = tokens
        q_send, kv_send = dense(0, False, True, hidden, **proj)
        for layer in range(layers):
            o = attention(q_send.reshape(XN, GRP, TOK, HD), kv_send)
            if layer + 1 < layers:
                hidden, q_send, kv_send = dense(layer, True, True, hidden, o=o, **ffn, **proj)
            else:
                hidden, = dense(layer, True, False, hidden, o=o, **ffn)
        return hidden

    return jax.shard_map(
        body,
        mesh=mesh5,
        in_specs=(row_spec, gain_spec, gain_spec, q_spec, col_spec, col_spec, o_spec, col_spec, col_spec, down_spec),
        out_specs=row_spec,
        check_vma=False,
    )
```

```python
import functools
import math
import jax
import jax.numpy as jnp
from jax import lax
from jax.experimental import pallas as pl
from jax.experimental.pallas import tpu as pltpu
from jax.sharding import Mesh, PartitionSpec as P

def seg_positions(dev_ids, rows, dev_total):
    offset = jnp.arange(rows)
    half_len = rows // 2
    seg_idx = jnp.where(offset < half_len, dev_ids[..., None], 2 * dev_total - 1 - dev_ids[..., None])
    return seg_idx * half_len + offset % half_len


SEG = 48
HD = 128
GRP = 3
XN = 4
SN = 16
RUN = XN * SEG
NRUN = 4
CH = NRUN * RUN
QR = GRP * RUN
TOK = 192
SCALE = math.log2(math.e) / math.sqrt(HD)
NB = 24
STRIP = 64


def quarter_block(quarter):
    return jnp.where(quarter == 0, 0, jnp.where(quarter == 1, 2, jnp.where(quarter == 2, 3, 1)))


def attn_kernel(q_send, kv_send, o_out, q_own, kv_all, o_own, o_recv, s_a, s_b, e_buf, m_ref, l_ref, acc_ref,
                send_a, recv_a, send_b, recv_b, send_o, recv_o):
    zi, yi, xi = lax.axis_index('z'), lax.axis_index('y'), lax.axis_index('x')
    group = zi * 4 + yi

    def slot(coords):
        return coords[0] * 4 + coords[1]

    def plus(v, d):
        return lax.rem(v + d + 4, 4)

    barrier = pltpu.get_barrier_semaphore()
    for d in (1, 2, 3):
        pl.semaphore_signal(barrier, inc=1, device_id={'x': plus(xi, d)}, device_id_type=pl.DeviceIdType.MESH)
    for d in (1, -1):
        pl.semaphore_signal(barrier, inc=1, device_id={'y': plus(yi, d)}, device_id_type=pl.DeviceIdType.MESH)
        pl.semaphore_signal(barrier, inc=1, device_id={'z': plus(zi, d)}, device_id_type=pl.DeviceIdType.MESH)
    pl.semaphore_wait(barrier, 7)

    def remote(src, dst, ssem, rsem, dev):
        return pltpu.make_async_remote_copy(src_ref=src, dst_ref=dst, send_sem=ssem, recv_sem=rsem, device_id=dev,
                                            device_id_type=pl.DeviceIdType.MESH)

    kv_msgs, q_msgs = {}, {}
    for d in (1, 3, 2):
        to = plus(xi, d)
        kv_msgs[d] = remote(kv_send.at[to], kv_all.at[group, 4 - d], send_a.at[d - 1], recv_a.at[d - 1], {'x': to})
        kv_msgs[d].start()
    for d in (1, 3, 2):
        to = plus(xi, d)
        q_msgs[d] = remote(q_send.at[to], q_own.at[xi], send_a.at[d + 2], recv_a.at[d + 2], {'x': to})

    pos = (zi, yi)
    names = ('z', 'y')

    def at(axis, da, db):
        other = 1 - axis
        c = [None, None]
        c[axis] = plus(pos[axis], da)
        c[other] = plus(pos[other], db)
        return slot(c)

    def msg(half, idx, where, part, axis, d):
        base = half * 2
        lo, n = (base, 2) if part is None else (base + part, 1)
        ref = kv_all.at[where, pl.ds(lo, n)]
        k = half * NB + idx
        return remote(ref, ref, send_b.at[k], recv_b.at[k], {names[axis]: plus(pos[axis], d)})

    first = (1, 0)
    stage = [dict() for _ in range(2)]
    offs = (0, -1, 1, 2)

    def begin(half, key, m):
        stage[half][key] = m
        m.start()

    def send_own(part):
        half, p = part // 2, part % 2
        a = first[half]
        src = kv_send.at[xi] if part == 0 else kv_all.at[group, part]
        for s, d in enumerate((1, -1)):
            for key, base, axis in (('a', 0, a), ('b0', 6, 1 - a)):
                k = half * NB + base + p * 2 + s
                begin(half, (key, p, d), remote(src, kv_all.at[group, part], send_b.at[k], recv_b.at[k],
                                                {names[axis]: plus(pos[axis], d)}))

    def send_second(half, j):
        a = first[half]
        b = 1 - a
        for s, d in enumerate((1, -1)):
            begin(half, ('b', j, d), msg(half, 8 + j * 4 + s, at(a, offs[j], 0), None, b, d))

    def forward_second(half, j):
        a = first[half]
        b = 1 - a
        for s, d in enumerate((1, -1)):
            stage[half][('b0', s, d) if j == 0 else ('b', j, d)].wait_recv()
            k = 10 + s if j == 0 else 10 + j * 4 + s
            begin(half, ('f', j, d), msg(half, k, at(a, offs[j], -d), s, b, d))
        if j == 0:
            for s, d in enumerate((1, -1)):
                stage[half][('b0', 1 - s, d)].wait_recv()

    Y, Z = 0, 1

    def forward_first(half):
        a = first[half]
        for s, d in enumerate((1, -1)):
            stage[half][('a', s, d)].wait_recv()
            begin(half, ('g', d), msg(half, 4 + s, at(a, -d, 0), s, a, d))
        for s, d in enumerate((1, -1)):
            stage[half][('a', 1 - s, d)].wait_recv()

    def got(half, *key):
        for d in (1, -1):
            stage[half][key + (d,)].wait_recv()

    def quarter_rows(t):
        desc = t >= 2
        return quarter_block(t), desc, [jnp.where(desc, XN - 1 - i, i) for i in range(XN)]

    def load_q(t):
        blk, _, xs = quarter_rows(t)
        row0 = pl.multiple_of(blk * SEG, 16)
        return jnp.concatenate([q_own[x, h, pl.ds(row0, SEG), :] for h in range(GRP) for x in xs], axis=0)

    def load_kv(kq, zr, which):
        blk, desc, xs = quarter_rows(kq)
        krow = pl.multiple_of(blk * SEG, 16)
        parts = []
        for r in range(NRUN):
            member = zr * 4 + jnp.where(desc, NRUN - 1 - r, r)
            for x in xs:
                parts.append(kv_all[member, plus(x, -xi), which, pl.ds(krow, SEG), :])
        return jnp.concatenate(parts, axis=0)

    def entry(e, lower, own):
        n0 = 4 if own else 2
        u = e - n0
        t = 1 + jnp.where(u >= 1, 1, 0) + jnp.where(u >= 3, 1, 0)
        kq = jnp.where(u < 1, 0, jnp.where(u < 3, u - 1, u - 3))
        t0 = e if own else jnp.where(lower, e, e + 2)
        return jnp.where(u < 0, t0, t), jnp.where(u < 0, t0, kq)

    def qk(tk, zr, s_ref, own):
        t, kq = tk
        s = lax.dot_general(load_q(t), load_kv(kq, zr, 0), (((1,), (1,)), ((), ())), preferred_element_type=jnp.float32)
        if own:
            row = lax.broadcasted_iota(jnp.int32, (RUN, CH), 0)
            col = lax.broadcasted_iota(jnp.int32, (RUN, CH), 1)
            mine = jnp.where(t >= 2, NRUN - 1 - yi, yi) * RUN
            visible = col <= row + jnp.where(t == kq, mine, CH)
            s = jnp.concatenate([jnp.where(visible, s[h * RUN:(h + 1) * RUN], -jnp.inf) for h in range(GRP)], axis=0)
        s_ref[...] = s

    def soft(tk, zr, s_ref):
        t, kq = tk
        vals = load_kv(kq, zr, 1)
        for h in range(GRP):
            for r0 in range(h * RUN, (h + 1) * RUN, STRIP):
                rows = slice(r0, r0 + STRIP)
                m_old = m_ref[t, rows, :]
                mx = s_ref[rows, 0:HD]
                for c in range(1, CH // HD):
                    mx = jnp.maximum(mx, s_ref[rows, c * HD:(c + 1) * HD])
                m_new = jnp.maximum(m_old, jnp.max(mx, axis=-1, keepdims=True))
                alpha = jnp.exp2((m_old - m_new) * SCALE)
                bias = m_new * SCALE
                lsum = l_ref[t, rows, :] * alpha
                for c in range(CH // HD):
                    e = jnp.exp2(s_ref[rows, c * HD:(c + 1) * HD] * SCALE - bias)
                    lsum = lsum + e
                    e_buf[rows, c * HD:(c + 1) * HD] = e.astype(jnp.bfloat16)
                m_ref[t, rows, :] = m_new
                l_ref[t, rows, :] = lsum
                acc_ref[t, rows, :] = acc_ref[t, rows, :] * alpha
            rows = slice(h * RUN, (h + 1) * RUN)
            acc_ref[t, rows, :] += jnp.dot(e_buf[rows, :], vals, preferred_element_type=jnp.float32)

    def run_row(zr, lower, own, lo, hi, after=None):
        n = 10 if own else 8
        if lo == 0:
            qk(entry(0, lower, own), zr, s_a, own)

        def pair(p, carry):
            qk(entry(2 * p + 1, lower, own), zr, s_b, own)
            soft(entry(2 * p, lower, own), zr, s_a)
            qk(entry(jnp.minimum(2 * p + 2, n - 1), lower, own), zr, s_a, own)
            soft(entry(2 * p + 1, lower, own), zr, s_b)
            if after is not None:
                after(p)
            return carry

        lax.fori_loop(lo, hi, pair, 0)

    def o_msg(step, d):
        to = plus(xi, d)
        blk = quarter_block(step)
        return remote(o_own.at[to, blk], o_recv.at[xi, blk], send_o.at[step, d - 1], recv_o.at[step, d - 1], {'x': to})

    def finish(t):
        blk, _, xs = quarter_rows(t)
        for h in range(GRP):
            rows = slice(h * RUN, (h + 1) * RUN)
            o = (acc_ref[t, rows, :] / jnp.sum(l_ref[t, rows, :], axis=-1, keepdims=True)).astype(jnp.bfloat16)
            for i in range(XN):
                o_own[xs[i], blk, h, :, :] = o[i * SEG:(i + 1) * SEG]
        for d in (2, 1, 3):
            o_msg(t, d).start()

    send_own(0)
    for d in (1, 3, 2):
        q_msgs[d].start()
    kv_all[group, 0] = kv_send[xi]
    q_own[xi] = q_send[xi]
    kv_msgs[3].wait_recv()
    send_own(1)
    kv_msgs[1].wait_recv()
    send_own(3)
    kv_msgs[2].wait_recv()
    send_own(2)
    m_ref[...] = jnp.full((4, QR, HD), -jnp.inf, jnp.float32)
    l_ref[...] = jnp.zeros((4, QR, HD), jnp.float32)
    acc_ref[...] = jnp.zeros((4, QR, HD), jnp.float32)
    forward_first(Y)
    send_second(Y, 1)
    send_second(Y, 2)
    forward_second(Z, 0)
    forward_first(Z)
    send_second(Z, 1)
    send_second(Z, 2)
    got(Y, 'g')
    send_second(Y, 3)
    forward_second(Y, 0)
    for c in q_msgs.values():
        c.wait_recv()
    got(Z, 'f', 0)
    rows_z = [plus(zi, d) for d in offs]
    lower = [r < zi for r in rows_z]
    run_row(zi, None, True, 0, 3)
    forward_second(Z, 1)
    forward_second(Y, 1)
    run_row(zi, None, True, 3, 5)
    forward_second(Z, 2)
    forward_second(Y, 2)
    got(Z, 'g')
    send_second(Z, 3)
    forward_second(Y, 3)
    got(Z, 'f', 1)
    run_row(rows_z[1], lower[1], False, 0, 4)
    forward_second(Z, 3)
    got(Z, 'f', 2)
    run_row(rows_z[2], lower[2], False, 0, 4)
    for j in range(4):
        got(Y, 'f', j)
    got(Z, 'f', 3)
    run_row(rows_z[3], lower[3], False, 0, 4, after=finish)
    o_recv[xi] = o_own[xi]
    for step in range(4):
        for d in (1, 2, 3):
            c = o_msg(step, d)
            c.wait_send()
            c.wait_recv()
    o_out[...] = o_recv[...]
    for c in list(kv_msgs.values()) + list(q_msgs.values()):
        c.wait_send()
    for half in range(2):
        for c in stage[half].values():
            c.wait_send()


def attention(q_send, kv_send):
    f32 = jnp.float32
    bf16 = jnp.bfloat16
    return pl.pallas_call(
        attn_kernel,
        out_shape=jax.ShapeDtypeStruct((XN, 4, GRP, SEG, HD), bf16),
        in_specs=[pl.BlockSpec(memory_space=pltpu.VMEM)] * 2,
        out_specs=pl.BlockSpec(memory_space=pltpu.VMEM),
        scratch_shapes=[
            pltpu.VMEM((XN, GRP, TOK, HD), bf16),
            pltpu.VMEM((SN, XN, 2, TOK, HD), bf16),
            pltpu.VMEM((XN, 4, GRP, SEG, HD), bf16),
            pltpu.VMEM((XN, 4, GRP, SEG, HD), bf16),
            pltpu.VMEM((QR, CH), f32),
            pltpu.VMEM((QR, CH), f32),
            pltpu.VMEM((QR, CH), bf16),
            pltpu.VMEM((4, QR, HD), f32),
            pltpu.VMEM((4, QR, HD), f32),
            pltpu.VMEM((4, QR, HD), f32),
            pltpu.SemaphoreType.DMA((6,)),
            pltpu.SemaphoreType.DMA((6,)),
            pltpu.SemaphoreType.DMA((2 * NB,)),
            pltpu.SemaphoreType.DMA((2 * NB,)),
            pltpu.SemaphoreType.DMA((4, 3)),
            pltpu.SemaphoreType.DMA((4, 3)),
        ],
        compiler_params=pltpu.CompilerParams(vmem_limit_bytes=40 << 20, collective_id=1, has_side_effects=True),
        cost_estimate=pl.CostEstimate(flops=2 * 2 * 130 * 192 * 576 * 128, bytes_accessed=8 << 20, transcendentals=0),
        name='attn',
    )(q_send, kv_send)


D = 3072
FF = 4096
ROWS = 96
NT = 512
NO = D // NT
NG = FF // NT
NS = 10


def dense_kernel(layer, post, qkv, *refs):
    refs = list(refs)
    hidden, norms = refs.pop(0), None
    if post:
        o_in, nm_mlp, w_o, w_g, w_u, w_d = refs[:6]
        refs = refs[6:]
    if qkv:
        nm_attn, cos_ref, sin_ref, w_q, w_k, w_v = refs[:6]
        refs = refs[6:]
    if post:
        hid_out = refs.pop(0)
    if qkv:
        q_out, kv_out = refs[:2]
        refs = refs[2:]
    wbuf, wsem = refs[:2]
    refs = refs[2:]
    if post:
        o_mat, hmid, nrm1, act, acc1, snd1, rcv1, acc2, snd2, rcv2, s1, r1, s2, r2 = refs[:14]
        refs = refs[14:]
    if qkv:
        nrm2 = refs.pop(0)
    sn, rn = refs
    t_me = lax.axis_index('tp')
    sibling = {'tp': 1 - t_me}

    n_o = NO if post else 0
    g0 = n_o
    d0 = g0 + (2 * NG if post else 0)
    q0 = d0 + (NO if post else 0)
    total = q0 + (5 if qkv else 0)

    def cols(i):
        return pl.ds(pl.multiple_of(i * NT, NT), NT)

    def copies(kind, i, slot):
        sem = wsem.at[slot]
        if kind == 'o':
            return [pltpu.make_async_copy(w_o.at[layer, :, cols(i)], wbuf.at[slot, pl.ds(0, 1536)], sem)]
        if kind == 'g':
            return [pltpu.make_async_copy(w_g.at[layer, :, cols(i)], wbuf.at[slot, pl.ds(0, D)], sem)]
        if kind == 'u':
            return [pltpu.make_async_copy(w_u.at[layer, :, cols(i)], wbuf.at[slot, pl.ds(0, D)], sem)]
        if kind == 'd':
            return [pltpu.make_async_copy(w_d.at[layer, :, cols(i)], wbuf.at[slot], sem)]
        nl = layer + 1 if post else layer
        if kind == 'q':
            return [pltpu.make_async_copy(w_q.at[nl, 4 * i + h], wbuf.at[slot, pl.ds(0, D), pl.ds(h * HD, HD)], sem)
                    for h in range(4)]
        if kind == 'k':
            return [pltpu.make_async_copy(w_k.at[nl], wbuf.at[slot, pl.ds(0, D)], sem)]
        return [pltpu.make_async_copy(w_v.at[nl], wbuf.at[slot, pl.ds(0, D)], sem)]

    def issue(t):
        slot = t % NS if isinstance(t, int) else lax.rem(t, NS)

        def go(cond, kind, i):
            if isinstance(cond, bool):
                if cond:
                    for c in copies(kind, i, slot):
                        c.start()
            else:
                @pl.when(cond)
                def _():
                    for c in copies(kind, i, slot):
                        c.start()

        def both(a, b):
            return (a and b) if isinstance(a, bool) else jnp.logical_and(a, b)

        if post:
            go(t < n_o, 'o', t)
            half = (t - g0) // 2
            even = (t - g0) % 2 == 0
            inside = both(t >= g0, t < d0)
            go(both(inside, even), 'g', half)
            go(both(inside, (t - g0) % 2 == 1), 'u', half)
            go(both(t >= d0, t < q0), 'd', t - d0)
        if qkv:
            go(both(t >= q0, t < q0 + 3), 'q', t - q0)
            go(t == q0 + 3, 'k', 0)
            go(t == q0 + 4, 'v', 0)

    def wait(t, depth):
        slot = t % NS if isinstance(t, int) else lax.rem(t, NS)
        ref = wbuf.at[slot, pl.ds(0, depth)]
        pltpu.make_async_copy(ref, ref, wsem.at[slot]).wait()
        return slot

    barrier = pltpu.get_barrier_semaphore()
    pl.semaphore_signal(barrier, inc=1, device_id=sibling, device_id_type=pl.DeviceIdType.MESH)
    for t in range(min(NS, total)):
        issue(t)

    def send(src, dst, ssem, rsem):
        return pltpu.make_async_remote_copy(src_ref=src, dst_ref=dst, send_sem=ssem, recv_sem=rsem, device_id=sibling,
                                            device_id_type=pl.DeviceIdType.MESH)

    def normed(src, gain_row, nrm, idx):
        ss = jnp.zeros((ROWS, 1), jnp.float32)
        for j in range(NO):
            v = src[:, j * NT:(j + 1) * NT].astype(jnp.float32)
            ss = ss + jnp.sum(v * v, axis=-1, keepdims=True)
        inv = lax.rsqrt(ss / D + 1e-5)
        for j in range(NO):
            sl = slice(j * NT, (j + 1) * NT)
            nrm[0:ROWS, sl] = (src[:, sl].astype(jnp.float32) * inv * gain_row[:, sl]).astype(jnp.bfloat16)
        c = send(nrm.at[pl.ds(0, ROWS)], nrm.at[pl.ds(ROWS, ROWS)], sn.at[idx], rn.at[idx])
        c.start()
        return c

    def part_copy(snd, rcv, ss, rs, i):
        return send(snd.at[i], rcv.at[i], ss.at[i], rs.at[i])

    def residual(base, acc, rcv, out, snd, ss, rs):
        for j in range(NO):
            part_copy(snd, rcv, ss, rs, j).wait_recv()
            sl = slice(j * NT, (j + 1) * NT)
            out[:, sl] = (base[:, sl].astype(jnp.float32) + (acc[j] + rcv[j])).astype(jnp.bfloat16)

    pending = []
    if post:
        for blk in range(4):
            row = pl.multiple_of(jnp.where(t_me == blk // 2, 0, ROWS) + (blk % 2) * SEG, 16)
            for x in range(XN):
                for h in range(GRP):
                    c0 = (x * GRP + h) * HD
                    o_mat[pl.ds(row, SEG), c0:c0 + HD] = o_in[x, blk, h]
        pl.semaphore_wait(barrier, 1)

        def o_step(i, carry):
            slot = wait(i, 1536)
            p = jnp.dot(o_mat[...], wbuf[slot, pl.ds(0, 1536), :], preferred_element_type=jnp.float32)
            acc1[i] = p[:ROWS]
            snd1[i] = p[ROWS:]
            part_copy(snd1, rcv1, s1, r1, i).start()
            issue(i + NS)
            return carry

        lax.fori_loop(0, NO, o_step, 0)
        residual(hidden, acc1, rcv1, hmid, snd1, s1, r1)
        c = normed(hmid, nm_mlp[...].astype(jnp.float32)[layer:layer + 1], nrm1, 0)
        c.wait_recv()
        pending.append(c)

        def g_step(i, carry):
            t = g0 + 2 * i
            slot_g = wait(t, D)
            g = jnp.dot(nrm1[...], wbuf[slot_g, pl.ds(0, D), :], preferred_element_type=jnp.float32)
            issue(t + NS)
            slot_u = wait(t + 1, D)
            u = jnp.dot(nrm1[...], wbuf[slot_u, pl.ds(0, D), :], preferred_element_type=jnp.float32)
            act[:, cols(i)] = (g * lax.logistic(g) * u).astype(jnp.bfloat16)
            issue(t + 1 + NS)
            return carry

        lax.fori_loop(0, NG, g_step, 0)

        def d_step(i, carry):
            slot = wait(d0 + i, FF)
            p = jnp.dot(act[...], wbuf[slot], preferred_element_type=jnp.float32)
            acc2[i] = p[:ROWS]
            snd2[i] = p[ROWS:]
            part_copy(snd2, rcv2, s2, r2, i).start()
            issue(d0 + i + NS)
            return carry

        lax.fori_loop(0, NO, d_step, 0)
        residual(hmid, acc2, rcv2, hid_out, snd2, s2, r2)
        cur = hid_out
    else:
        pl.semaphore_wait(barrier, 1)
        cur = hidden
    if qkv:
        nl = layer + 1 if post else layer
        c = normed(cur, nm_attn[...].astype(jnp.float32)[nl:nl + 1], nrm2, 1)
        c.wait_recv()
        pending.append(c)
        mine = pl.ds(pl.multiple_of(t_me * ROWS, 16), ROWS)
        theirs = pl.ds(pl.multiple_of((1 - t_me) * ROWS, 16), ROWS)

        def project(t):
            slot = wait(t, D)
            return jnp.dot(nrm2[...], wbuf[slot, pl.ds(0, D), :], preferred_element_type=jnp.float32)

        def rotate(v):
            return v * cos_ref[...] + pltpu.roll(v, HD // 2, 1) * sin_ref[...]

        def q_step(i, carry):
            p = project(q0 + i)
            for h in range(4):
                r = rotate(p[:, h * HD:(h + 1) * HD]).astype(jnp.bfloat16)
                q_out[4 * i + h, mine, :] = r[:ROWS]
                q_out[4 * i + h, theirs, :] = r[ROWS:]
            return carry

        lax.fori_loop(0, 3, q_step, 0)
        for which in range(2):
            p = project(q0 + 3 + which)
            for h in range(4):
                r = p[:, h * HD:(h + 1) * HD]
                r = (rotate(r) if which == 0 else r).astype(jnp.bfloat16)
                kv_out[h, which, mine, :] = r[:ROWS]
                kv_out[h, which, theirs, :] = r[ROWS:]
    for c in pending:
        c.wait_send()
    if post:
        for i in range(NO):
            part_copy(snd1, rcv1, s1, r1, i).wait_send()
            part_copy(snd2, rcv2, s2, r2, i).wait_send()


def dense(layer, post, qkv, hidden, o=None, norm_mlp=None, w_o=None, w_g=None, w_u=None, w_d=None, norm_attn=None, cos_t=None,
          sin_t=None, w_q=None, w_k=None, w_v=None):
    f32, bf16 = jnp.float32, jnp.bfloat16
    vmem = pl.BlockSpec(memory_space=pltpu.VMEM)
    hbm = pl.BlockSpec(memory_space=pltpu.HBM)
    args, specs, outs, scratch = [hidden], [vmem], [], []
    if post:
        args += [o, norm_mlp, w_o, w_g, w_u, w_d]
        specs += [vmem, vmem] + [hbm] * 4
        outs.append(jax.ShapeDtypeStruct((ROWS, D), bf16))
    if qkv:
        args += [norm_attn, cos_t, sin_t, w_q, w_k, w_v]
        specs += [vmem] * 3 + [hbm] * 3
        outs += [jax.ShapeDtypeStruct((XN * GRP, TOK, HD), bf16), jax.ShapeDtypeStruct((XN, 2, TOK, HD), bf16)]
    scratch += [pltpu.VMEM((NS, FF, NT), bf16), pltpu.SemaphoreType.DMA((NS,))]
    if post:
        part = pltpu.VMEM((NO, ROWS, NT), f32)
        scratch += [pltpu.VMEM((TOK, 1536), bf16), pltpu.VMEM((ROWS, D), bf16), pltpu.VMEM((TOK, D), bf16),
                    pltpu.VMEM((TOK, FF), bf16)] + [part] * 6 + [pltpu.SemaphoreType.DMA((NO,))] * 4
    if qkv:
        scratch += [pltpu.VMEM((TOK, D), bf16)]
    scratch += [pltpu.SemaphoreType.DMA((2,))] * 2
    moved = (85 << 20 if post else 0) + (16 << 20 if qkv else 0)
    return pl.pallas_call(
        functools.partial(dense_kernel, layer, post, qkv),
        out_shape=tuple(outs),
        in_specs=specs,
        out_specs=tuple([vmem] * len(outs)),
        scratch_shapes=scratch,
        compiler_params=pltpu.CompilerParams(vmem_limit_bytes=63 << 20, collective_id=2 + layer + (1 if post else 0),
                                             has_side_effects=True),
        cost_estimate=pl.CostEstimate(flops=TOK * moved, bytes_accessed=moved, transcendentals=0),
        name=f'dense{layer}{int(post)}{int(qkv)}',
    )(*args)


def solution(mesh):
    tp_size = mesh.shape['tp']
    cp_size = mesh.shape['cp']
    dev_total = tp_size * cp_size
    mesh5 = Mesh(mesh.devices.reshape(1, tp_size, 4, 4, 4), ('dp', 'tp', 'z', 'y', 'x'))
    row_spec = P(('dp', 'tp', 'z', 'y', 'x'), None)
    gain_spec = P(None, None)
    q_spec = P(None, None, 'tp', None)
    col_spec = P(None, None, 'tp')
    o_spec = P(None, 'tp', None, None)
    down_spec = P(None, 'tp', None)

    def body(tokens, norm_attn, norm_mlp, w_q, w_k, w_v, w_o, w_gate, w_up, w_down):
        rows = tokens.shape[0]
        tp_idx = lax.axis_index('tp')
        cp_idx = (lax.axis_index('z') * 4 + lax.axis_index('y')) * 4 + lax.axis_index('x')
        tp_devs = jnp.stack([tp_idx, 1 - tp_idx]) * cp_size + cp_idx
        pos = seg_positions(tp_devs, rows, dev_total).reshape(tp_size * rows)
        inv_freq = 500000.0 ** (-(jnp.arange(HD // 2, dtype=jnp.float32) * 2.0 / HD))
        angles = pos.astype(jnp.float32)[:, None] * inv_freq[None, :]
        cos_a, sin_a = jnp.cos(angles), jnp.sin(angles)
        cos_t = jnp.concatenate([cos_a, cos_a], axis=1)
        sin_t = jnp.concatenate([-sin_a, sin_a], axis=1)
        layers = w_q.shape[0]
        proj = dict(norm_attn=norm_attn, cos_t=cos_t, sin_t=sin_t, w_q=w_q.transpose(0, 2, 1, 3), w_k=w_k, w_v=w_v)
        ffn = dict(norm_mlp=norm_mlp, w_o=w_o.reshape(layers, -1, D), w_g=w_gate, w_u=w_up, w_d=w_down)
        hidden = tokens
        q_send, kv_send = dense(0, False, True, hidden, **proj)
        for layer in range(layers):
            o = attention(q_send.reshape(XN, GRP, TOK, HD), kv_send)
            if layer + 1 < layers:
                hidden, q_send, kv_send = dense(layer, True, True, hidden, o=o, **ffn, **proj)
            else:
                hidden, = dense(layer, True, False, hidden, o=o, **ffn)
        return hidden

    return jax.shard_map(
        body,
        mesh=mesh5,
        in_specs=(row_spec, gain_spec, gain_spec, q_spec, col_spec, col_spec, o_spec, col_spec, col_spec, down_spec),
        out_specs=row_spec,
        check_vma=False,
    )
```

```python
import functools
import math
import jax
import jax.numpy as jnp
from jax import lax
from jax.experimental import pallas as pl
from jax.experimental.pallas import tpu as pltpu
from jax.sharding import Mesh, PartitionSpec as P

def seg_positions(dev_ids, rows, dev_total):
    offset = jnp.arange(rows)
    half_len = rows // 2
    seg_idx = jnp.where(offset < half_len, dev_ids[..., None], 2 * dev_total - 1 - dev_ids[..., None])
    return seg_idx * half_len + offset % half_len


SEG = 48
HD = 128
GRP = 3
XN = 4
SN = 16
RUN = XN * SEG
NRUN = 4
CH = NRUN * RUN
QR = GRP * RUN
TOK = 192
SCALE = math.log2(math.e) / math.sqrt(HD)
NB = 24
STRIP = 64


def quarter_block(quarter):
    return jnp.where(quarter == 0, 0, jnp.where(quarter == 1, 2, jnp.where(quarter == 2, 3, 1)))


def attend(fill, q_send, kv_send, q_own, kv_all, o_own, o_recv, s_a, s_b, e_buf, m_ref, l_ref, acc_ref,
                send_a, recv_a, send_b, recv_b, send_o, recv_o):
    zi, yi, xi = lax.axis_index('z'), lax.axis_index('y'), lax.axis_index('x')
    group = zi * 4 + yi

    def slot(coords):
        return coords[0] * 4 + coords[1]

    def plus(v, d):
        return lax.rem(v + d + 4, 4)

    barrier = pltpu.get_barrier_semaphore()
    for d in (1, 2, 3):
        pl.semaphore_signal(barrier, inc=1, device_id={'x': plus(xi, d)}, device_id_type=pl.DeviceIdType.MESH)
    for d in (1, -1):
        pl.semaphore_signal(barrier, inc=1, device_id={'y': plus(yi, d)}, device_id_type=pl.DeviceIdType.MESH)
        pl.semaphore_signal(barrier, inc=1, device_id={'z': plus(zi, d)}, device_id_type=pl.DeviceIdType.MESH)
    pl.semaphore_signal(barrier, inc=1, device_id={'tp': 1 - lax.axis_index('tp')}, device_id_type=pl.DeviceIdType.MESH)
    fill()
    pl.semaphore_wait(barrier, 8)

    def remote(src, dst, ssem, rsem, dev):
        return pltpu.make_async_remote_copy(src_ref=src, dst_ref=dst, send_sem=ssem, recv_sem=rsem, device_id=dev,
                                            device_id_type=pl.DeviceIdType.MESH)

    kv_msgs, q_msgs = {}, {}
    for d in (1, 3, 2):
        to = plus(xi, d)
        kv_msgs[d] = remote(kv_send.at[to], kv_all.at[group, 4 - d], send_a.at[d - 1], recv_a.at[d - 1], {'x': to})
        kv_msgs[d].start()
    for d in (1, 3, 2):
        to = plus(xi, d)
        q_msgs[d] = remote(q_send.at[to], q_own.at[xi], send_a.at[d + 2], recv_a.at[d + 2], {'x': to})

    pos = (zi, yi)
    names = ('z', 'y')

    def at(axis, da, db):
        other = 1 - axis
        c = [None, None]
        c[axis] = plus(pos[axis], da)
        c[other] = plus(pos[other], db)
        return slot(c)

    def msg(half, idx, where, part, axis, d):
        base = half * 2
        lo, n = (base, 2) if part is None else (base + part, 1)
        ref = kv_all.at[where, pl.ds(lo, n)]
        k = half * NB + idx
        return remote(ref, ref, send_b.at[k], recv_b.at[k], {names[axis]: plus(pos[axis], d)})

    first = (1, 0)
    stage = [dict() for _ in range(2)]
    offs = (0, -1, 1, 2)

    def begin(half, key, m):
        stage[half][key] = m
        m.start()

    def send_own(part):
        half, p = part // 2, part % 2
        a = first[half]
        src = kv_send.at[xi] if part == 0 else kv_all.at[group, part]
        for s, d in enumerate((1, -1)):
            for key, base, axis in (('a', 0, a), ('b0', 6, 1 - a)):
                k = half * NB + base + p * 2 + s
                begin(half, (key, p, d), remote(src, kv_all.at[group, part], send_b.at[k], recv_b.at[k],
                                                {names[axis]: plus(pos[axis], d)}))

    def send_second(half, j):
        a = first[half]
        b = 1 - a
        for s, d in enumerate((1, -1)):
            begin(half, ('b', j, d), msg(half, 8 + j * 4 + s, at(a, offs[j], 0), None, b, d))

    def forward_second(half, j):
        a = first[half]
        b = 1 - a
        for s, d in enumerate((1, -1)):
            stage[half][('b0', s, d) if j == 0 else ('b', j, d)].wait_recv()
            k = 10 + s if j == 0 else 10 + j * 4 + s
            begin(half, ('f', j, d), msg(half, k, at(a, offs[j], -d), s, b, d))
        if j == 0:
            for s, d in enumerate((1, -1)):
                stage[half][('b0', 1 - s, d)].wait_recv()

    Y, Z = 0, 1

    def forward_first(half):
        a = first[half]
        for s, d in enumerate((1, -1)):
            stage[half][('a', s, d)].wait_recv()
            begin(half, ('g', d), msg(half, 4 + s, at(a, -d, 0), s, a, d))
        for s, d in enumerate((1, -1)):
            stage[half][('a', 1 - s, d)].wait_recv()

    def got(half, *key):
        for d in (1, -1):
            stage[half][key + (d,)].wait_recv()

    def quarter_rows(t):
        desc = t >= 2
        return quarter_block(t), desc, [jnp.where(desc, XN - 1 - i, i) for i in range(XN)]

    def load_q(t):
        blk, _, xs = quarter_rows(t)
        row0 = pl.multiple_of(blk * SEG, 16)
        return jnp.concatenate([q_own[x, h, pl.ds(row0, SEG), :] for h in range(GRP) for x in xs], axis=0)

    def load_kv(kq, zr, which):
        blk, desc, xs = quarter_rows(kq)
        krow = pl.multiple_of(blk * SEG, 16)
        parts = []
        for r in range(NRUN):
            member = zr * 4 + jnp.where(desc, NRUN - 1 - r, r)
            for x in xs:
                parts.append(kv_all[member, plus(x, -xi), which, pl.ds(krow, SEG), :])
        return jnp.concatenate(parts, axis=0)

    def entry(e, lower, own):
        n0 = 4 if own else 2
        u = e - n0
        t = 1 + jnp.where(u >= 1, 1, 0) + jnp.where(u >= 3, 1, 0)
        kq = jnp.where(u < 1, 0, jnp.where(u < 3, u - 1, u - 3))
        t0 = e if own else jnp.where(lower, e, e + 2)
        return jnp.where(u < 0, t0, t), jnp.where(u < 0, t0, kq)

    def qk(tk, zr, s_ref, own):
        t, kq = tk
        s = lax.dot_general(load_q(t), load_kv(kq, zr, 0), (((1,), (1,)), ((), ())), preferred_element_type=jnp.float32)
        if own:
            row = lax.broadcasted_iota(jnp.int32, (RUN, CH), 0)
            col = lax.broadcasted_iota(jnp.int32, (RUN, CH), 1)
            mine = jnp.where(t >= 2, NRUN - 1 - yi, yi) * RUN
            visible = col <= row + jnp.where(t == kq, mine, CH)
            s = jnp.concatenate([jnp.where(visible, s[h * RUN:(h + 1) * RUN], -jnp.inf) for h in range(GRP)], axis=0)
        s_ref[...] = s

    def soft(tk, zr, s_ref):
        t, kq = tk
        vals = load_kv(kq, zr, 1)
        for h in range(GRP):
            for r0 in range(h * RUN, (h + 1) * RUN, STRIP):
                rows = slice(r0, r0 + STRIP)
                m_old = m_ref[t, rows, :]
                mx = s_ref[rows, 0:HD]
                for c in range(1, CH // HD):
                    mx = jnp.maximum(mx, s_ref[rows, c * HD:(c + 1) * HD])
                m_new = jnp.maximum(m_old, jnp.max(mx, axis=-1, keepdims=True))
                alpha = jnp.exp2((m_old - m_new) * SCALE)
                bias = m_new * SCALE
                lsum = l_ref[t, rows, :] * alpha
                for c in range(CH // HD):
                    e = jnp.exp2(s_ref[rows, c * HD:(c + 1) * HD] * SCALE - bias)
                    lsum = lsum + e
                    e_buf[rows, c * HD:(c + 1) * HD] = e.astype(jnp.bfloat16)
                m_ref[t, rows, :] = m_new
                l_ref[t, rows, :] = lsum
                acc_ref[t, rows, :] = acc_ref[t, rows, :] * alpha
            rows = slice(h * RUN, (h + 1) * RUN)
            acc_ref[t, rows, :] += jnp.dot(e_buf[rows, :], vals, preferred_element_type=jnp.float32)

    def run_row(zr, lower, own, lo, hi, after=None):
        n = 10 if own else 8
        if lo == 0:
            qk(entry(0, lower, own), zr, s_a, own)

        def pair(p, carry):
            qk(entry(2 * p + 1, lower, own), zr, s_b, own)
            soft(entry(2 * p, lower, own), zr, s_a)
            qk(entry(jnp.minimum(2 * p + 2, n - 1), lower, own), zr, s_a, own)
            soft(entry(2 * p + 1, lower, own), zr, s_b)
            if after is not None:
                after(p)
            return carry

        lax.fori_loop(lo, hi, pair, 0)

    def o_msg(step, d):
        to = plus(xi, d)
        blk = quarter_block(step)
        return remote(o_own.at[to, blk], o_recv.at[xi, blk], send_o.at[step, d - 1], recv_o.at[step, d - 1], {'x': to})

    def finish(t):
        blk, _, xs = quarter_rows(t)
        for h in range(GRP):
            rows = slice(h * RUN, (h + 1) * RUN)
            o = (acc_ref[t, rows, :] / jnp.sum(l_ref[t, rows, :], axis=-1, keepdims=True)).astype(jnp.bfloat16)
            for i in range(XN):
                o_own[xs[i], blk, h, :, :] = o[i * SEG:(i + 1) * SEG]
        for d in (2, 1, 3):
            o_msg(t, d).start()

    send_own(0)
    for d in (1, 3, 2):
        q_msgs[d].start()
    kv_all[group, 0] = kv_send[xi]
    q_own[xi] = q_send[xi]
    kv_msgs[3].wait_recv()
    send_own(1)
    kv_msgs[1].wait_recv()
    send_own(3)
    kv_msgs[2].wait_recv()
    send_own(2)
    m_ref[...] = jnp.full((4, QR, HD), -jnp.inf, jnp.float32)
    l_ref[...] = jnp.zeros((4, QR, HD), jnp.float32)
    acc_ref[...] = jnp.zeros((4, QR, HD), jnp.float32)
    forward_first(Y)
    send_second(Y, 1)
    send_second(Y, 2)
    forward_second(Z, 0)
    forward_first(Z)
    send_second(Z, 1)
    send_second(Z, 2)
    got(Y, 'g')
    send_second(Y, 3)
    forward_second(Y, 0)
    for c in q_msgs.values():
        c.wait_recv()
    got(Z, 'f', 0)
    rows_z = [plus(zi, d) for d in offs]
    lower = [r < zi for r in rows_z]
    run_row(zi, None, True, 0, 3)
    forward_second(Z, 1)
    forward_second(Y, 1)
    run_row(zi, None, True, 3, 5)
    forward_second(Z, 2)
    forward_second(Y, 2)
    got(Z, 'g')
    send_second(Z, 3)
    forward_second(Y, 3)
    got(Z, 'f', 1)
    run_row(rows_z[1], lower[1], False, 0, 4)
    forward_second(Z, 3)
    got(Z, 'f', 2)
    run_row(rows_z[2], lower[2], False, 0, 4)
    for j in range(4):
        got(Y, 'f', j)
    got(Z, 'f', 3)
    run_row(rows_z[3], lower[3], False, 0, 4, after=finish)
    o_recv[xi] = o_own[xi]
    for step in range(4):
        for d in (1, 2, 3):
            c = o_msg(step, d)
            c.wait_send()
            c.wait_recv()
    for c in list(kv_msgs.values()) + list(q_msgs.values()):
        c.wait_send()
    for half in range(2):
        for c in stage[half].values():
            c.wait_send()


def attn_scratch():
    f32 = jnp.float32
    bf16 = jnp.bfloat16
    return [
        pltpu.VMEM((XN, GRP, TOK, HD), bf16),
        pltpu.VMEM((SN, XN, 2, TOK, HD), bf16),
        pltpu.VMEM((XN, 4, GRP, SEG, HD), bf16),
        pltpu.VMEM((XN, 4, GRP, SEG, HD), bf16),
        pltpu.VMEM((QR, CH), f32),
        pltpu.VMEM((QR, CH), f32),
        pltpu.VMEM((QR, CH), bf16),
        pltpu.VMEM((4, QR, HD), f32),
        pltpu.VMEM((4, QR, HD), f32),
        pltpu.VMEM((4, QR, HD), f32),
        pltpu.SemaphoreType.DMA((6,)),
        pltpu.SemaphoreType.DMA((6,)),
        pltpu.SemaphoreType.DMA((2 * NB,)),
        pltpu.SemaphoreType.DMA((2 * NB,)),
        pltpu.SemaphoreType.DMA((4, 3)),
        pltpu.SemaphoreType.DMA((4, 3)),
    ]


D = 3072
FF = 4096
ROWS = 96
NT = 512
NO = D // NT
NG = FF // NT
NS = 7


def dense_kernel(layer, post, qkv, *refs):
    refs = list(refs)
    hidden, norms = refs.pop(0), None
    if post:
        q_send, kv_send, nm_mlp, w_o, w_g, w_u, w_d = refs[:7]
        refs = refs[7:]
    if qkv:
        nm_attn, cos_ref, sin_ref, w_q, w_k, w_v = refs[:6]
        refs = refs[6:]
    if post:
        hid_out = refs.pop(0)
    if qkv:
        q_out, kv_out = refs[:2]
        refs = refs[2:]
    wbuf, wsem = refs[:2]
    refs = refs[2:]
    if post:
        attn_refs, refs = refs[:16], refs[16:]
        o_in = attn_refs[3]
        o_mat, hmid, nrm1, act, acc1, snd1, rcv1, acc2, snd2, rcv2, s1, r1, s2, r2 = refs[:14]
        refs = refs[14:]
    if qkv:
        nrm2 = refs.pop(0)
    sn, rn = refs
    t_me = lax.axis_index('tp')
    sibling = {'tp': 1 - t_me}

    n_o = NO // 2 if post else 0
    g0 = n_o
    d0 = g0 + (2 * NG if post else 0)
    q0 = d0 + (NO if post else 0)
    total = q0 + (5 if qkv else 0)

    def cols(i):
        return pl.ds(pl.multiple_of(i * NT, NT), NT)

    def copies(kind, i, slot):
        sem = wsem.at[slot]
        if kind == 'o':
            return [pltpu.make_async_copy(w_o.at[layer, :, cols(2 * i + p)], wbuf.at[slot, pl.ds(p * 1536, 1536)], sem)
                    for p in range(2)]
        if kind == 'g':
            return [pltpu.make_async_copy(w_g.at[layer, :, cols(i)], wbuf.at[slot, pl.ds(0, D)], sem)]
        if kind == 'u':
            return [pltpu.make_async_copy(w_u.at[layer, :, cols(i)], wbuf.at[slot, pl.ds(0, D)], sem)]
        if kind == 'd':
            return [pltpu.make_async_copy(w_d.at[layer, :, cols(i)], wbuf.at[slot], sem)]
        nl = layer + 1 if post else layer
        if kind == 'q':
            return [pltpu.make_async_copy(w_q.at[nl, 4 * i + h], wbuf.at[slot, pl.ds(0, D), pl.ds(h * HD, HD)], sem)
                    for h in range(4)]
        if kind == 'k':
            return [pltpu.make_async_copy(w_k.at[nl], wbuf.at[slot, pl.ds(0, D)], sem)]
        return [pltpu.make_async_copy(w_v.at[nl], wbuf.at[slot, pl.ds(0, D)], sem)]

    def issue(t):
        slot = t % NS if isinstance(t, int) else lax.rem(t, NS)

        def go(cond, kind, i):
            if isinstance(cond, bool):
                if cond:
                    for c in copies(kind, i, slot):
                        c.start()
            else:
                @pl.when(cond)
                def _():
                    for c in copies(kind, i, slot):
                        c.start()

        def both(a, b):
            return (a and b) if isinstance(a, bool) else jnp.logical_and(a, b)

        if post:
            go(t < n_o, 'o', t)
            half = (t - g0) // 2
            even = (t - g0) % 2 == 0
            inside = both(t >= g0, t < d0)
            go(both(inside, even), 'g', half)
            go(both(inside, (t - g0) % 2 == 1), 'u', half)
            go(both(t >= d0, t < q0), 'd', t - d0)
        if qkv:
            go(both(t >= q0, t < q0 + 3), 'q', t - q0)
            go(t == q0 + 3, 'k', 0)
            go(t == q0 + 4, 'v', 0)

    def wait(t, depth):
        slot = t % NS if isinstance(t, int) else lax.rem(t, NS)
        ref = wbuf.at[slot, pl.ds(0, depth)]
        pltpu.make_async_copy(ref, ref, wsem.at[slot]).wait()
        return slot

    def fill():
        for t in range(min(NS, total)):
            issue(t)

    if post:
        attend(fill, q_send, kv_send, *attn_refs)
    else:
        barrier = pltpu.get_barrier_semaphore()
        pl.semaphore_signal(barrier, inc=1, device_id=sibling, device_id_type=pl.DeviceIdType.MESH)
        fill()

    def send(src, dst, ssem, rsem):
        return pltpu.make_async_remote_copy(src_ref=src, dst_ref=dst, send_sem=ssem, recv_sem=rsem, device_id=sibling,
                                            device_id_type=pl.DeviceIdType.MESH)

    def normed(src, gain_row, nrm, idx):
        ss = jnp.zeros((ROWS, 1), jnp.float32)
        for j in range(NO):
            v = src[:, j * NT:(j + 1) * NT].astype(jnp.float32)
            ss = ss + jnp.sum(v * v, axis=-1, keepdims=True)
        inv = lax.rsqrt(ss / D + 1e-5)
        for j in range(NO):
            sl = slice(j * NT, (j + 1) * NT)
            nrm[0:ROWS, sl] = (src[:, sl].astype(jnp.float32) * inv * gain_row[:, sl]).astype(jnp.bfloat16)
        c = send(nrm.at[pl.ds(0, ROWS)], nrm.at[pl.ds(ROWS, ROWS)], sn.at[idx], rn.at[idx])
        c.start()
        return c

    def part_copy(snd, rcv, ss, rs, i):
        return send(snd.at[i], rcv.at[i], ss.at[i], rs.at[i])

    def residual(base, acc, rcv, out, snd, ss, rs):
        for j in range(NO):
            part_copy(snd, rcv, ss, rs, j).wait_recv()
            sl = slice(j * NT, (j + 1) * NT)
            out[:, sl] = (base[:, sl].astype(jnp.float32) + (acc[j] + rcv[j])).astype(jnp.bfloat16)

    pending = []
    if post:
        for blk in range(4):
            row = pl.multiple_of(jnp.where(t_me == blk // 2, 0, ROWS) + (blk % 2) * SEG, 16)
            for x in range(XN):
                for h in range(GRP):
                    c0 = (x * GRP + h) * HD
                    o_mat[pl.ds(row, SEG), c0:c0 + HD] = o_in[x, blk, h]

        def o_step(i, carry):
            slot = wait(i, D)
            for q in range(2):
                p = jnp.dot(o_mat[...], wbuf[slot, pl.ds(q * 1536, 1536), :], preferred_element_type=jnp.float32)
                acc1[2 * i + q] = p[:ROWS]
                snd1[2 * i + q] = p[ROWS:]
                part_copy(snd1, rcv1, s1, r1, 2 * i + q).start()
            issue(i + NS)
            return carry

        lax.fori_loop(0, NO // 2, o_step, 0)
        residual(hidden, acc1, rcv1, hmid, snd1, s1, r1)
        c = normed(hmid, nm_mlp[...].astype(jnp.float32)[layer:layer + 1], nrm1, 0)
        c.wait_recv()
        pending.append(c)

        def g_step(i, carry):
            t = g0 + 2 * i
            slot_g = wait(t, D)
            g = jnp.dot(nrm1[...], wbuf[slot_g, pl.ds(0, D), :], preferred_element_type=jnp.float32)
            issue(t + NS)
            slot_u = wait(t + 1, D)
            u = jnp.dot(nrm1[...], wbuf[slot_u, pl.ds(0, D), :], preferred_element_type=jnp.float32)
            act[:, cols(i)] = (g * lax.logistic(g) * u).astype(jnp.bfloat16)
            issue(t + 1 + NS)
            return carry

        lax.fori_loop(0, NG, g_step, 0)

        def d_step(i, carry):
            slot = wait(d0 + i, FF)
            p = jnp.dot(act[...], wbuf[slot], preferred_element_type=jnp.float32)
            acc2[i] = p[:ROWS]
            snd2[i] = p[ROWS:]
            part_copy(snd2, rcv2, s2, r2, i).start()
            issue(d0 + i + NS)
            return carry

        lax.fori_loop(0, NO, d_step, 0)
        residual(hmid, acc2, rcv2, hid_out, snd2, s2, r2)
        cur = hid_out
    else:
        pl.semaphore_wait(barrier, 1)
        cur = hidden
    if qkv:
        nl = layer + 1 if post else layer
        c = normed(cur, nm_attn[...].astype(jnp.float32)[nl:nl + 1], nrm2, 1)
        c.wait_recv()
        pending.append(c)
        mine = pl.ds(pl.multiple_of(t_me * ROWS, 16), ROWS)
        theirs = pl.ds(pl.multiple_of((1 - t_me) * ROWS, 16), ROWS)

        def project(t):
            slot = wait(t, D)
            return jnp.dot(nrm2[...], wbuf[slot, pl.ds(0, D), :], preferred_element_type=jnp.float32)

        def rotate(v):
            return v * cos_ref[...] + pltpu.roll(v, HD // 2, 1) * sin_ref[...]

        def q_step(i, carry):
            p = project(q0 + i)
            for h in range(4):
                r = rotate(p[:, h * HD:(h + 1) * HD]).astype(jnp.bfloat16)
                q_out[4 * i + h, mine, :] = r[:ROWS]
                q_out[4 * i + h, theirs, :] = r[ROWS:]
            return carry

        lax.fori_loop(0, 3, q_step, 0)
        for which in range(2):
            p = project(q0 + 3 + which)
            for h in range(4):
                r = p[:, h * HD:(h + 1) * HD]
                r = (rotate(r) if which == 0 else r).astype(jnp.bfloat16)
                kv_out[h, which, mine, :] = r[:ROWS]
                kv_out[h, which, theirs, :] = r[ROWS:]
    for c in pending:
        c.wait_send()
    if post:
        for i in range(NO):
            part_copy(snd1, rcv1, s1, r1, i).wait_send()
            part_copy(snd2, rcv2, s2, r2, i).wait_send()


def dense(layer, post, qkv, hidden, q_send=None, kv_send=None, norm_mlp=None, w_o=None, w_g=None, w_u=None, w_d=None, norm_attn=None, cos_t=None,
          sin_t=None, w_q=None, w_k=None, w_v=None):
    f32, bf16 = jnp.float32, jnp.bfloat16
    vmem = pl.BlockSpec(memory_space=pltpu.VMEM)
    hbm = pl.BlockSpec(memory_space=pltpu.HBM)
    args, specs, outs, scratch = [hidden], [vmem], [], []
    if post:
        args += [q_send, kv_send, norm_mlp, w_o, w_g, w_u, w_d]
        specs += [vmem] * 3 + [hbm] * 4
        outs.append(jax.ShapeDtypeStruct((ROWS, D), bf16))
    if qkv:
        args += [norm_attn, cos_t, sin_t, w_q, w_k, w_v]
        specs += [vmem] * 3 + [hbm] * 3
        outs += [jax.ShapeDtypeStruct((XN * GRP, TOK, HD), bf16), jax.ShapeDtypeStruct((XN, 2, TOK, HD), bf16)]
    scratch += [pltpu.VMEM((NS, FF, NT), bf16), pltpu.SemaphoreType.DMA((NS,))]
    if post:
        part = pltpu.VMEM((NO, ROWS, NT), f32)
        scratch += attn_scratch() + [pltpu.VMEM((TOK, 1536), bf16), pltpu.VMEM((ROWS, D), bf16), pltpu.VMEM((TOK, D), bf16),
                    pltpu.VMEM((TOK, FF), bf16)] + [part] * 6 + [pltpu.SemaphoreType.DMA((NO,))] * 4
    if qkv:
        scratch += [pltpu.VMEM((TOK, D), bf16)]
    scratch += [pltpu.SemaphoreType.DMA((2,))] * 2
    moved = (85 << 20 if post else 0) + (16 << 20 if qkv else 0)
    return pl.pallas_call(
        functools.partial(dense_kernel, layer, post, qkv),
        out_shape=tuple(outs),
        in_specs=specs,
        out_specs=tuple([vmem] * len(outs)),
        scratch_shapes=scratch,
        compiler_params=pltpu.CompilerParams(vmem_limit_bytes=67043328, collective_id=2 + layer + (1 if post else 0),
                                             has_side_effects=True),
        cost_estimate=pl.CostEstimate(flops=TOK * moved, bytes_accessed=moved, transcendentals=0),
        name=f'dense{layer}{int(post)}{int(qkv)}',
    )(*args)


def solution(mesh):
    tp_size = mesh.shape['tp']
    cp_size = mesh.shape['cp']
    dev_total = tp_size * cp_size
    mesh5 = Mesh(mesh.devices.reshape(1, tp_size, 4, 4, 4), ('dp', 'tp', 'z', 'y', 'x'))
    row_spec = P(('dp', 'tp', 'z', 'y', 'x'), None)
    gain_spec = P(None, None)
    q_spec = P(None, None, 'tp', None)
    col_spec = P(None, None, 'tp')
    o_spec = P(None, 'tp', None, None)
    down_spec = P(None, 'tp', None)

    def body(tokens, norm_attn, norm_mlp, w_q, w_k, w_v, w_o, w_gate, w_up, w_down):
        rows = tokens.shape[0]
        tp_idx = lax.axis_index('tp')
        cp_idx = (lax.axis_index('z') * 4 + lax.axis_index('y')) * 4 + lax.axis_index('x')
        tp_devs = jnp.stack([tp_idx, 1 - tp_idx]) * cp_size + cp_idx
        pos = seg_positions(tp_devs, rows, dev_total).reshape(tp_size * rows)
        inv_freq = 500000.0 ** (-(jnp.arange(HD // 2, dtype=jnp.float32) * 2.0 / HD))
        angles = pos.astype(jnp.float32)[:, None] * inv_freq[None, :]
        cos_a, sin_a = jnp.cos(angles), jnp.sin(angles)
        cos_t = jnp.concatenate([cos_a, cos_a], axis=1)
        sin_t = jnp.concatenate([-sin_a, sin_a], axis=1)
        layers = w_q.shape[0]
        proj = dict(norm_attn=norm_attn, cos_t=cos_t, sin_t=sin_t, w_q=w_q.transpose(0, 2, 1, 3), w_k=w_k, w_v=w_v)
        ffn = dict(norm_mlp=norm_mlp, w_o=w_o.reshape(layers, -1, D), w_g=w_gate, w_u=w_up, w_d=w_down)
        hidden = tokens
        q_send, kv_send = dense(0, False, True, hidden, **proj)
        for layer in range(layers):
            q_send = q_send.reshape(XN, GRP, TOK, HD)
            if layer + 1 < layers:
                hidden, q_send, kv_send = dense(layer, True, True, hidden, q_send=q_send, kv_send=kv_send, **ffn, **proj)
            else:
                hidden, = dense(layer, True, False, hidden, q_send=q_send, kv_send=kv_send, **ffn)
        return hidden

    return jax.shard_map(
        body,
        mesh=mesh5,
        in_specs=(row_spec, gain_spec, gain_spec, q_spec, col_spec, col_spec, o_spec, col_spec, col_spec, down_spec),
        out_specs=row_spec,
        check_vma=False,
    )
```

```python
import functools
import math
import jax
import jax.numpy as jnp
from jax import lax
from jax.experimental import pallas as pl
from jax.experimental.pallas import tpu as pltpu
from jax.sharding import Mesh, PartitionSpec as P

def seg_positions(dev_ids, rows, dev_total):
    offset = jnp.arange(rows)
    half_len = rows // 2
    seg_idx = jnp.where(offset < half_len, dev_ids[..., None], 2 * dev_total - 1 - dev_ids[..., None])
    return seg_idx * half_len + offset % half_len


SEG = 48
HD = 128
GRP = 3
XN = 4
SN = 16
RUN = XN * SEG
NRUN = 4
CH = NRUN * RUN
QR = GRP * RUN
TOK = 192
SCALE = math.log2(math.e) / math.sqrt(HD)
NB = 24
STRIP = 64


def quarter_block(quarter):
    return jnp.where(quarter == 0, 0, jnp.where(quarter == 1, 2, jnp.where(quarter == 2, 3, 1)))


def attend(fill, q_send, kv_send, q_own, kv_all, o_own, o_recv, s_a, s_b, e_buf, m_ref, l_ref, acc_ref,
                send_a, recv_a, send_b, recv_b, send_o, recv_o):
    zi, yi, xi = lax.axis_index('z'), lax.axis_index('y'), lax.axis_index('x')
    group = zi * 4 + yi

    def slot(coords):
        return coords[0] * 4 + coords[1]

    def plus(v, d):
        return lax.rem(v + d + 4, 4)

    barrier = pltpu.get_barrier_semaphore()
    for d in (1, 2, 3):
        pl.semaphore_signal(barrier, inc=1, device_id={'x': plus(xi, d)}, device_id_type=pl.DeviceIdType.MESH)
    for d in (1, -1):
        pl.semaphore_signal(barrier, inc=1, device_id={'y': plus(yi, d)}, device_id_type=pl.DeviceIdType.MESH)
        pl.semaphore_signal(barrier, inc=1, device_id={'z': plus(zi, d)}, device_id_type=pl.DeviceIdType.MESH)
    pl.semaphore_signal(barrier, inc=1, device_id={'tp': 1 - lax.axis_index('tp')}, device_id_type=pl.DeviceIdType.MESH)
    fill()
    pl.semaphore_wait(barrier, 8)

    def remote(src, dst, ssem, rsem, dev):
        return pltpu.make_async_remote_copy(src_ref=src, dst_ref=dst, send_sem=ssem, recv_sem=rsem, device_id=dev,
                                            device_id_type=pl.DeviceIdType.MESH)

    kv_msgs, q_msgs = {}, {}
    for d in (1, 3, 2):
        to = plus(xi, d)
        kv_msgs[d] = remote(kv_send.at[to], kv_all.at[group, 4 - d], send_a.at[d - 1], recv_a.at[d - 1], {'x': to})
        kv_msgs[d].start()
    for d in (1, 3, 2):
        to = plus(xi, d)
        q_msgs[d] = remote(q_send.at[to], q_own.at[xi], send_a.at[d + 2], recv_a.at[d + 2], {'x': to})

    pos = (zi, yi)
    names = ('z', 'y')

    def at(axis, da, db):
        other = 1 - axis
        c = [None, None]
        c[axis] = plus(pos[axis], da)
        c[other] = plus(pos[other], db)
        return slot(c)

    def msg(half, idx, where, part, axis, d):
        base = half * 2
        lo, n = (base, 2) if part is None else (base + part, 1)
        ref = kv_all.at[where, pl.ds(lo, n)]
        k = half * NB + idx
        return remote(ref, ref, send_b.at[k], recv_b.at[k], {names[axis]: plus(pos[axis], d)})

    first = (1, 0)
    stage = [dict() for _ in range(2)]
    offs = (0, -1, 1, 2)

    def begin(half, key, m):
        stage[half][key] = m
        m.start()

    def send_own(part):
        half, p = part // 2, part % 2
        a = first[half]
        src = kv_send.at[xi] if part == 0 else kv_all.at[group, part]
        for s, d in enumerate((1, -1)):
            for key, base, axis in (('a', 0, a), ('b0', 6, 1 - a)):
                k = half * NB + base + p * 2 + s
                begin(half, (key, p, d), remote(src, kv_all.at[group, part], send_b.at[k], recv_b.at[k],
                                                {names[axis]: plus(pos[axis], d)}))

    def send_second(half, j):
        a = first[half]
        b = 1 - a
        for s, d in enumerate((1, -1)):
            begin(half, ('b', j, d), msg(half, 8 + j * 4 + s, at(a, offs[j], 0), None, b, d))

    def forward_second(half, j):
        a = first[half]
        b = 1 - a
        for s, d in enumerate((1, -1)):
            stage[half][('b0', s, d) if j == 0 else ('b', j, d)].wait_recv()
            k = 10 + s if j == 0 else 10 + j * 4 + s
            begin(half, ('f', j, d), msg(half, k, at(a, offs[j], -d), s, b, d))
        if j == 0:
            for s, d in enumerate((1, -1)):
                stage[half][('b0', 1 - s, d)].wait_recv()

    Y, Z = 0, 1

    def forward_first(half):
        a = first[half]
        for s, d in enumerate((1, -1)):
            stage[half][('a', s, d)].wait_recv()
            begin(half, ('g', d), msg(half, 4 + s, at(a, -d, 0), s, a, d))
        for s, d in enumerate((1, -1)):
            stage[half][('a', 1 - s, d)].wait_recv()

    def got(half, *key):
        for d in (1, -1):
            stage[half][key + (d,)].wait_recv()

    def quarter_rows(t):
        desc = t >= 2
        return quarter_block(t), desc, [jnp.where(desc, XN - 1 - i, i) for i in range(XN)]

    def load_q(t):
        blk, _, xs = quarter_rows(t)
        row0 = pl.multiple_of(blk * SEG, 16)
        return jnp.concatenate([q_own[x, h, pl.ds(row0, SEG), :] for h in range(GRP) for x in xs], axis=0)

    def load_kv(kq, zr, which):
        blk, desc, xs = quarter_rows(kq)
        krow = pl.multiple_of(blk * SEG, 16)
        parts = []
        for r in range(NRUN):
            member = zr * 4 + jnp.where(desc, NRUN - 1 - r, r)
            for x in xs:
                parts.append(kv_all[member, plus(x, -xi), which, pl.ds(krow, SEG), :])
        return jnp.concatenate(parts, axis=0)

    def entry(e, lower, own):
        n0 = 4 if own else 2
        u = e - n0
        t = 1 + jnp.where(u >= 1, 1, 0) + jnp.where(u >= 3, 1, 0)
        kq = jnp.where(u < 1, 0, jnp.where(u < 3, u - 1, u - 3))
        t0 = e if own else jnp.where(lower, e, e + 2)
        return jnp.where(u < 0, t0, t), jnp.where(u < 0, t0, kq)

    def qk(tk, zr, s_ref, own):
        t, kq = tk
        s = lax.dot_general(load_q(t), load_kv(kq, zr, 0), (((1,), (1,)), ((), ())), preferred_element_type=jnp.float32)
        if own:
            row = lax.broadcasted_iota(jnp.int32, (RUN, CH), 0)
            col = lax.broadcasted_iota(jnp.int32, (RUN, CH), 1)
            mine = jnp.where(t >= 2, NRUN - 1 - yi, yi) * RUN
            visible = col <= row + jnp.where(t == kq, mine, CH)
            s = jnp.concatenate([jnp.where(visible, s[h * RUN:(h + 1) * RUN], -jnp.inf) for h in range(GRP)], axis=0)
        s_ref[...] = s

    def soft(tk, zr, s_ref):
        t, kq = tk
        vals = load_kv(kq, zr, 1)
        for h in range(GRP):
            for r0 in range(h * RUN, (h + 1) * RUN, STRIP):
                rows = slice(r0, r0 + STRIP)
                m_old = m_ref[t, rows, :]
                mx = s_ref[rows, 0:HD]
                for c in range(1, CH // HD):
                    mx = jnp.maximum(mx, s_ref[rows, c * HD:(c + 1) * HD])
                m_new = jnp.maximum(m_old, jnp.max(mx, axis=-1, keepdims=True))
                alpha = jnp.exp2((m_old - m_new) * SCALE)
                bias = m_new * SCALE
                lsum = l_ref[t, rows, :] * alpha
                for c in range(CH // HD):
                    e = jnp.exp2(s_ref[rows, c * HD:(c + 1) * HD] * SCALE - bias)
                    lsum = lsum + e
                    e_buf[rows, c * HD:(c + 1) * HD] = e.astype(jnp.bfloat16)
                m_ref[t, rows, :] = m_new
                l_ref[t, rows, :] = lsum
                acc_ref[t, rows, :] = acc_ref[t, rows, :] * alpha
            rows = slice(h * RUN, (h + 1) * RUN)
            acc_ref[t, rows, :] += jnp.dot(e_buf[rows, :], vals, preferred_element_type=jnp.float32)

    def run_row(zr, lower, own, lo, hi, after=None):
        n = 10 if own else 8
        if lo == 0:
            qk(entry(0, lower, own), zr, s_a, own)

        def pair(p, carry):
            qk(entry(2 * p + 1, lower, own), zr, s_b, own)
            soft(entry(2 * p, lower, own), zr, s_a)
            qk(entry(jnp.minimum(2 * p + 2, n - 1), lower, own), zr, s_a, own)
            soft(entry(2 * p + 1, lower, own), zr, s_b)
            if after is not None:
                after(p)
            return carry

        lax.fori_loop(lo, hi, pair, 0)

    def o_msg(step, d):
        to = plus(xi, d)
        blk = quarter_block(step)
        return remote(o_own.at[to, blk], o_recv.at[xi, blk], send_o.at[step, d - 1], recv_o.at[step, d - 1], {'x': to})

    def finish(t):
        blk, _, xs = quarter_rows(t)
        for h in range(GRP):
            rows = slice(h * RUN, (h + 1) * RUN)
            o = (acc_ref[t, rows, :] / jnp.sum(l_ref[t, rows, :], axis=-1, keepdims=True)).astype(jnp.bfloat16)
            for i in range(XN):
                o_own[xs[i], blk, h, :, :] = o[i * SEG:(i + 1) * SEG]
        for d in (2, 1, 3):
            o_msg(t, d).start()

    send_own(0)
    for d in (1, 3, 2):
        q_msgs[d].start()
    kv_all[group, 0] = kv_send[xi]
    q_own[xi] = q_send[xi]
    kv_msgs[3].wait_recv()
    send_own(1)
    kv_msgs[1].wait_recv()
    send_own(3)
    kv_msgs[2].wait_recv()
    send_own(2)
    m_ref[...] = jnp.full((4, QR, HD), -jnp.inf, jnp.float32)
    l_ref[...] = jnp.zeros((4, QR, HD), jnp.float32)
    acc_ref[...] = jnp.zeros((4, QR, HD), jnp.float32)
    forward_first(Y)
    send_second(Y, 1)
    send_second(Y, 2)
    forward_second(Z, 0)
    forward_first(Z)
    send_second(Z, 1)
    send_second(Z, 2)
    got(Y, 'g')
    send_second(Y, 3)
    forward_second(Y, 0)
    for c in q_msgs.values():
        c.wait_recv()
    got(Z, 'f', 0)
    rows_z = [plus(zi, d) for d in offs]
    lower = [r < zi for r in rows_z]
    run_row(zi, None, True, 0, 3)
    forward_second(Z, 1)
    forward_second(Y, 1)
    run_row(zi, None, True, 3, 5)
    forward_second(Z, 2)
    forward_second(Y, 2)
    got(Z, 'g')
    send_second(Z, 3)
    forward_second(Y, 3)
    got(Z, 'f', 1)
    run_row(rows_z[1], lower[1], False, 0, 4)
    forward_second(Z, 3)
    got(Z, 'f', 2)
    run_row(rows_z[2], lower[2], False, 0, 4)
    for j in range(4):
        got(Y, 'f', j)
    got(Z, 'f', 3)
    run_row(rows_z[3], lower[3], False, 0, 4, after=finish)
    o_recv[xi] = o_own[xi]
    for step in range(4):
        for d in (1, 2, 3):
            c = o_msg(step, d)
            c.wait_send()
            c.wait_recv()
    for c in list(kv_msgs.values()) + list(q_msgs.values()):
        c.wait_send()
    for half in range(2):
        for c in stage[half].values():
            c.wait_send()


def attn_scratch():
    f32 = jnp.float32
    bf16 = jnp.bfloat16
    return [
        pltpu.VMEM((XN, GRP, TOK, HD), bf16),
        pltpu.VMEM((SN, XN, 2, TOK, HD), bf16),
        pltpu.VMEM((XN, 4, GRP, SEG, HD), bf16),
        pltpu.VMEM((XN, 4, GRP, SEG, HD), bf16),
        pltpu.VMEM((QR, CH), f32),
        pltpu.VMEM((QR, CH), f32),
        pltpu.VMEM((QR, CH), bf16),
        pltpu.VMEM((4, QR, HD), f32),
        pltpu.VMEM((4, QR, HD), f32),
        pltpu.VMEM((4, QR, HD), f32),
        pltpu.SemaphoreType.DMA((6,)),
        pltpu.SemaphoreType.DMA((6,)),
        pltpu.SemaphoreType.DMA((2 * NB,)),
        pltpu.SemaphoreType.DMA((2 * NB,)),
        pltpu.SemaphoreType.DMA((4, 3)),
        pltpu.SemaphoreType.DMA((4, 3)),
    ]


D = 3072
FF = 4096
ROWS = 96
NT = 512
NO = D // NT
NG = FF // NT
NS = 7


def dense_kernel(layer, post, qkv, *refs):
    refs = list(refs)
    hidden, norms = refs.pop(0), None
    if post:
        q_send, kv_send, nm_mlp, w_o, w_g, w_u, w_d = refs[:7]
        refs = refs[7:]
    if qkv:
        nm_attn, cos_ref, sin_ref, w_q, w_k, w_v = refs[:6]
        refs = refs[6:]
    if post:
        hid_out = refs.pop(0)
    if qkv:
        q_out, kv_out = refs[:2]
        refs = refs[2:]
    wbuf, wsem = refs[:2]
    refs = refs[2:]
    if post:
        attn_refs, refs = refs[:16], refs[16:]
        o_in = attn_refs[3]
        o_mat, hmid, nrm1, act, acc1, snd1, rcv1, acc2, snd2, rcv2, s1, r1, s2, r2 = refs[:14]
        refs = refs[14:]
    if qkv:
        nrm2 = refs.pop(0)
    sn, rn = refs
    t_me = lax.axis_index('tp')
    sibling = {'tp': 1 - t_me}

    n_o = NO // 2 if post else 0
    g0 = n_o
    d0 = g0 + (2 * NG if post else 0)
    q0 = d0 + (NO if post else 0)
    total = q0 + (5 if qkv else 0)

    def cols(i):
        return pl.ds(pl.multiple_of(i * NT, NT), NT)

    def copies(kind, i, slot):
        sem = wsem.at[slot]
        if kind == 'o':
            return [pltpu.make_async_copy(w_o.at[layer, :, cols(2 * i + p)], wbuf.at[slot, pl.ds(p * 1536, 1536)], sem)
                    for p in range(2)]
        if kind == 'g':
            return [pltpu.make_async_copy(w_g.at[layer, :, cols(i)], wbuf.at[slot, pl.ds(0, D)], sem)]
        if kind == 'u':
            return [pltpu.make_async_copy(w_u.at[layer, :, cols(i)], wbuf.at[slot, pl.ds(0, D)], sem)]
        if kind == 'd':
            return [pltpu.make_async_copy(w_d.at[layer, :, cols(i)], wbuf.at[slot], sem)]
        nl = layer + 1 if post else layer
        if kind == 'q':
            return [pltpu.make_async_copy(w_q.at[nl, 4 * i + h], wbuf.at[slot, pl.ds(0, D), pl.ds(h * HD, HD)], sem)
                    for h in range(4)]
        if kind == 'k':
            return [pltpu.make_async_copy(w_k.at[nl], wbuf.at[slot, pl.ds(0, D)], sem)]
        return [pltpu.make_async_copy(w_v.at[nl], wbuf.at[slot, pl.ds(0, D)], sem)]

    def issue(t):
        slot = t % NS if isinstance(t, int) else lax.rem(t, NS)

        def go(cond, kind, i):
            if isinstance(cond, bool):
                if cond:
                    for c in copies(kind, i, slot):
                        c.start()
            else:
                @pl.when(cond)
                def _():
                    for c in copies(kind, i, slot):
                        c.start()

        def both(a, b):
            return (a and b) if isinstance(a, bool) else jnp.logical_and(a, b)

        if post:
            go(t < n_o, 'o', t)
            half = (t - g0) // 2
            even = (t - g0) % 2 == 0
            inside = both(t >= g0, t < d0)
            go(both(inside, even), 'g', half)
            go(both(inside, (t - g0) % 2 == 1), 'u', half)
            go(both(t >= d0, t < q0), 'd', t - d0)
        if qkv:
            go(both(t >= q0, t < q0 + 3), 'q', t - q0)
            go(t == q0 + 3, 'k', 0)
            go(t == q0 + 4, 'v', 0)

    def wait(t, depth):
        slot = t % NS if isinstance(t, int) else lax.rem(t, NS)
        ref = wbuf.at[slot, pl.ds(0, depth)]
        pltpu.make_async_copy(ref, ref, wsem.at[slot]).wait()
        return slot

    def fill():
        for t in range(min(NS, total)):
            issue(t)

    if post:
        attend(fill, q_send, kv_send, *attn_refs)
    else:
        barrier = pltpu.get_barrier_semaphore()
        pl.semaphore_signal(barrier, inc=1, device_id=sibling, device_id_type=pl.DeviceIdType.MESH)
        fill()

    def send(src, dst, ssem, rsem):
        return pltpu.make_async_remote_copy(src_ref=src, dst_ref=dst, send_sem=ssem, recv_sem=rsem, device_id=sibling,
                                            device_id_type=pl.DeviceIdType.MESH)

    pending = []

    def normed(src, gain_row, nrm, idx):
        ss = jnp.zeros((ROWS, 1), jnp.float32)
        for j in range(NO):
            v = src[:, j * NT:(j + 1) * NT].astype(jnp.float32)
            ss = ss + jnp.sum(v * v, axis=-1, keepdims=True)
        inv = lax.rsqrt(ss / D + 1e-5)
        for j in range(NO):
            sl = slice(j * NT, (j + 1) * NT)
            nrm[0:ROWS, sl] = (src[:, sl].astype(jnp.float32) * inv * gain_row[:, sl]).astype(jnp.bfloat16)
            part = pl.ds(j * NT, NT)
            c = send(nrm.at[pl.ds(0, ROWS), part], nrm.at[pl.ds(ROWS, ROWS), part], sn.at[idx, j], rn.at[idx, j])
            c.start()
            pending.append(c)
        for c in pending[-NO:]:
            c.wait_recv()

    def part_copy(snd, rcv, ss, rs, i):
        return send(snd.at[i], rcv.at[i], ss.at[i], rs.at[i])

    def residual(base, acc, rcv, out, snd, ss, rs):
        for j in range(NO):
            part_copy(snd, rcv, ss, rs, j).wait_recv()
            sl = slice(j * NT, (j + 1) * NT)
            out[:, sl] = (base[:, sl].astype(jnp.float32) + (acc[j] + rcv[j])).astype(jnp.bfloat16)

    if post:
        for blk in range(4):
            row = pl.multiple_of(jnp.where(t_me == blk // 2, 0, ROWS) + (blk % 2) * SEG, 16)
            for x in range(XN):
                for h in range(GRP):
                    c0 = (x * GRP + h) * HD
                    o_mat[pl.ds(row, SEG), c0:c0 + HD] = o_in[x, blk, h]

        def o_step(i, carry):
            slot = wait(i, D)
            for q in range(2):
                p = jnp.dot(o_mat[...], wbuf[slot, pl.ds(q * 1536, 1536), :], preferred_element_type=jnp.float32)
                acc1[2 * i + q] = p[:ROWS]
                snd1[2 * i + q] = p[ROWS:]
                part_copy(snd1, rcv1, s1, r1, 2 * i + q).start()
            issue(i + NS)
            return carry

        lax.fori_loop(0, NO // 2, o_step, 0)
        residual(hidden, acc1, rcv1, hmid, snd1, s1, r1)
        normed(hmid, nm_mlp[...].astype(jnp.float32)[layer:layer + 1], nrm1, 0)

        def g_step(i, carry):
            t = g0 + 2 * i
            slot_g = wait(t, D)
            g = jnp.dot(nrm1[...], wbuf[slot_g, pl.ds(0, D), :], preferred_element_type=jnp.float32)
            issue(t + NS)
            slot_u = wait(t + 1, D)
            u = jnp.dot(nrm1[...], wbuf[slot_u, pl.ds(0, D), :], preferred_element_type=jnp.float32)
            act[:, cols(i)] = (g * lax.logistic(g) * u).astype(jnp.bfloat16)
            issue(t + 1 + NS)
            return carry

        lax.fori_loop(0, NG, g_step, 0)

        def d_step(i, carry):
            slot = wait(d0 + i, FF)
            p = jnp.dot(act[...], wbuf[slot], preferred_element_type=jnp.float32)
            acc2[i] = p[:ROWS]
            snd2[i] = p[ROWS:]
            part_copy(snd2, rcv2, s2, r2, i).start()
            issue(d0 + i + NS)
            return carry

        lax.fori_loop(0, NO, d_step, 0)
        residual(hmid, acc2, rcv2, hid_out, snd2, s2, r2)
        cur = hid_out
    else:
        pl.semaphore_wait(barrier, 1)
        cur = hidden
    if qkv:
        nl = layer + 1 if post else layer
        normed(cur, nm_attn[...].astype(jnp.float32)[nl:nl + 1], nrm2, 1)
        mine = pl.ds(pl.multiple_of(t_me * ROWS, 16), ROWS)
        theirs = pl.ds(pl.multiple_of((1 - t_me) * ROWS, 16), ROWS)

        def project(t):
            slot = wait(t, D)
            return jnp.dot(nrm2[...], wbuf[slot, pl.ds(0, D), :], preferred_element_type=jnp.float32)

        def rotate(v):
            return v * cos_ref[...] + pltpu.roll(v, HD // 2, 1) * sin_ref[...]

        def q_step(i, carry):
            p = project(q0 + i)
            for h in range(4):
                r = rotate(p[:, h * HD:(h + 1) * HD]).astype(jnp.bfloat16)
                q_out[4 * i + h, mine, :] = r[:ROWS]
                q_out[4 * i + h, theirs, :] = r[ROWS:]
            return carry

        lax.fori_loop(0, 3, q_step, 0)
        for which in range(2):
            p = project(q0 + 3 + which)
            for h in range(4):
                r = p[:, h * HD:(h + 1) * HD]
                r = (rotate(r) if which == 0 else r).astype(jnp.bfloat16)
                kv_out[h, which, mine, :] = r[:ROWS]
                kv_out[h, which, theirs, :] = r[ROWS:]
    for c in pending:
        c.wait_send()
    if post:
        for i in range(NO):
            part_copy(snd1, rcv1, s1, r1, i).wait_send()
            part_copy(snd2, rcv2, s2, r2, i).wait_send()


def dense(layer, post, qkv, hidden, q_send=None, kv_send=None, norm_mlp=None, w_o=None, w_g=None, w_u=None, w_d=None, norm_attn=None, cos_t=None,
          sin_t=None, w_q=None, w_k=None, w_v=None):
    f32, bf16 = jnp.float32, jnp.bfloat16
    vmem = pl.BlockSpec(memory_space=pltpu.VMEM)
    hbm = pl.BlockSpec(memory_space=pltpu.HBM)
    args, specs, outs, scratch = [hidden], [vmem], [], []
    if post:
        args += [q_send, kv_send, norm_mlp, w_o, w_g, w_u, w_d]
        specs += [vmem] * 3 + [hbm] * 4
        outs.append(jax.ShapeDtypeStruct((ROWS, D), bf16))
    if qkv:
        args += [norm_attn, cos_t, sin_t, w_q, w_k, w_v]
        specs += [vmem] * 3 + [hbm] * 3
        outs += [jax.ShapeDtypeStruct((XN * GRP, TOK, HD), bf16), jax.ShapeDtypeStruct((XN, 2, TOK, HD), bf16)]
    scratch += [pltpu.VMEM((NS, FF, NT), bf16), pltpu.SemaphoreType.DMA((NS,))]
    if post:
        part = pltpu.VMEM((NO, ROWS, NT), f32)
        scratch += attn_scratch() + [pltpu.VMEM((TOK, 1536), bf16), pltpu.VMEM((ROWS, D), bf16), pltpu.VMEM((TOK, D), bf16),
                    pltpu.VMEM((TOK, FF), bf16)] + [part] * 6 + [pltpu.SemaphoreType.DMA((NO,))] * 4
    if qkv:
        scratch += [pltpu.VMEM((TOK, D), bf16)]
    scratch += [pltpu.SemaphoreType.DMA((2, NO))] * 2
    moved = (85 << 20 if post else 0) + (16 << 20 if qkv else 0)
    return pl.pallas_call(
        functools.partial(dense_kernel, layer, post, qkv),
        out_shape=tuple(outs),
        in_specs=specs,
        out_specs=tuple([vmem] * len(outs)),
        scratch_shapes=scratch,
        compiler_params=pltpu.CompilerParams(vmem_limit_bytes=67043328, collective_id=2 + layer + (1 if post else 0),
                                             has_side_effects=True),
        cost_estimate=pl.CostEstimate(flops=TOK * moved, bytes_accessed=moved, transcendentals=0),
        name=f'dense{layer}{int(post)}{int(qkv)}',
    )(*args)


def solution(mesh):
    tp_size = mesh.shape['tp']
    cp_size = mesh.shape['cp']
    dev_total = tp_size * cp_size
    mesh5 = Mesh(mesh.devices.reshape(1, tp_size, 4, 4, 4), ('dp', 'tp', 'z', 'y', 'x'))
    row_spec = P(('dp', 'tp', 'z', 'y', 'x'), None)
    gain_spec = P(None, None)
    q_spec = P(None, None, 'tp', None)
    col_spec = P(None, None, 'tp')
    o_spec = P(None, 'tp', None, None)
    down_spec = P(None, 'tp', None)

    def body(tokens, norm_attn, norm_mlp, w_q, w_k, w_v, w_o, w_gate, w_up, w_down):
        rows = tokens.shape[0]
        tp_idx = lax.axis_index('tp')
        cp_idx = (lax.axis_index('z') * 4 + lax.axis_index('y')) * 4 + lax.axis_index('x')
        tp_devs = jnp.stack([tp_idx, 1 - tp_idx]) * cp_size + cp_idx
        pos = seg_positions(tp_devs, rows, dev_total).reshape(tp_size * rows)
        inv_freq = 500000.0 ** (-(jnp.arange(HD // 2, dtype=jnp.float32) * 2.0 / HD))
        angles = pos.astype(jnp.float32)[:, None] * inv_freq[None, :]
        cos_a, sin_a = jnp.cos(angles), jnp.sin(angles)
        cos_t = jnp.concatenate([cos_a, cos_a], axis=1)
        sin_t = jnp.concatenate([-sin_a, sin_a], axis=1)
        layers = w_q.shape[0]
        proj = dict(norm_attn=norm_attn, cos_t=cos_t, sin_t=sin_t, w_q=w_q.transpose(0, 2, 1, 3), w_k=w_k, w_v=w_v)
        ffn = dict(norm_mlp=norm_mlp, w_o=w_o.reshape(layers, -1, D), w_g=w_gate, w_u=w_up, w_d=w_down)
        hidden = tokens
        q_send, kv_send = dense(0, False, True, hidden, **proj)
        for layer in range(layers):
            q_send = q_send.reshape(XN, GRP, TOK, HD)
            if layer + 1 < layers:
                hidden, q_send, kv_send = dense(layer, True, True, hidden, q_send=q_send, kv_send=kv_send, **ffn, **proj)
            else:
                hidden, = dense(layer, True, False, hidden, q_send=q_send, kv_send=kv_send, **ffn)
        return hidden

    return jax.shard_map(
        body,
        mesh=mesh5,
        in_specs=(row_spec, gain_spec, gain_spec, q_spec, col_spec, col_spec, o_spec, col_spec, col_spec, down_spec),
        out_specs=row_spec,
        check_vma=False,
    )
```
